32 devices in a mesh: dp: 4 (over x, core), ep: 8 (over z, y).
Axes of the slice: x: 2, y: 2, z: 4, core: 2. Of those that a mesh axis runs over, the one named last changes fastest.
Arguments:
- tokens: bfloat16 [4096, 7168], P(('dp', 'ep')), may hold values from -6 to 6
- out_grad: bfloat16 [4096, 7168], P(('dp', 'ep')), may hold values from -3 to 3
- expert_ids: int32 [4096, 8], P(('dp', 'ep')), may hold values from 0 to 255, as said below
- route_weights: bfloat16 [4096, 8], P(('dp', 'ep')), may hold values from 0.099609375 to 1
- gate_matrix: bfloat16 [7168, 2048], P('dp', 'ep'), may hold values from -0.0625 to 0.0625
- up_matrix: bfloat16 [7168, 2048], P('dp', 'ep'), may hold values from -0.0625 to 0.0625
- down_matrix: bfloat16 [7168, 2048], P('dp', 'ep'), may hold values from -0.125 to 0.125
Outputs:
- input_gradient: bfloat16 [4096, 7168], P(('dp', 'ep'))
- route_gradient: float32 [4096, 8], P(('dp', 'ep'))
- gate_gradient: bfloat16 [7168, 2048], P('dp', 'ep')
- up_gradient: bfloat16 [7168, 2048], P('dp', 'ep')
- down_gradient: bfloat16 [7168, 2048], P('dp', 'ep')
The draws below stay inside these ranges and needn't reach their ends.
Inputs may be any that keep to these rules, and one draw needn't show every extreme that they name: `expert_ids`: each row names 8 different ids, 2 in each of 4 groups of 32 consecutive ids. In each aligned block of 1024 rows, one id that is a multiple of 256 is named by 8 or more rows of every aligned block of 128 rows inside it.
All inputs are finite; a program needn't handle non-finite values.
Results may differ from the reference program's by a relative error of at most 0.014.
Values may be sent and summed in bfloat16 or wider, within the bound.
A program may use at most 128 MiB of HBM per device.

```python
import math
import jax
import jax.numpy as jnp
from jax import lax

D = 7168
FF = 2048
ROUTED = 256
NGROUPS = 8
TOPG = 4
TOPK = 8
SLICES = 8
TOK_DEV = 128
HID_DEV = 256
EXPERTS = 1
STRIDE = 256
CAP = 8
TOKENS = 4096
N_DP = 4
N_EP = 8


def draw_expert_ids(key, part):
    total_rows = TOK_DEV * N_EP * N_DP
    group_width = ROUTED // NGROUPS
    per_group = TOPK // TOPG
    base = jax.random.fold_in(key, 7)
    key_hot = jax.random.fold_in(base, 1)
    key_groups = jax.random.fold_in(base, 2)
    key_members = jax.random.fold_in(base, 3)
    hottest = jax.random.randint(key_hot, (N_DP,), 0, EXPERTS) * STRIDE
    row_index = jnp.arange(total_rows, dtype=jnp.int32)
    forced = row_index % TOK_DEV < CAP
    hot_expert = hottest[row_index // (TOK_DEV * N_EP)]
    hot_group = hot_expert // group_width
    group_index = jnp.arange(NGROUPS, dtype=jnp.int32)
    group_scores = jax.random.randint(key_groups, (total_rows, NGROUPS), 0, 4096) * NGROUPS + group_index[None, :]
    group_scores = group_scores + jnp.where(forced[:, None] & (group_index[None, :] == hot_group[:, None]), 1 << 24, 0)
    chosen_groups = lax.top_k(group_scores, TOPG)[1].astype(jnp.int32)
    member_index = jnp.arange(group_width, dtype=jnp.int32)
    candidates = chosen_groups[:, :, None] * group_width + member_index[None, None, :]
    member_scores = jax.random.randint(key_members, (total_rows, TOPG, group_width), 0, 4096) * group_width + member_index[None, None, :]
    member_scores = member_scores + jnp.where(forced[:, None, None] & (candidates == hot_expert[:, None, None]), 1 << 24, 0)
    picked = lax.top_k(member_scores, per_group)[1]
    chosen = jnp.take_along_axis(candidates, picked, axis=2)
    return chosen.reshape(total_rows, TOPK).astype(jnp.int32)


def levels(rng, extent, cuts, smallest, high):
    factor_of, own = 1.0, jax.random.fold_in(rng, 6)
    for axis_at, parts in cuts:
        steps = jnp.exp(jax.random.uniform(jax.random.fold_in(own, axis_at), (parts,), jnp.float32, smallest / len(cuts), high / len(cuts)))
        factor_of = factor_of * jnp.repeat(steps, extent[axis_at] // parts).reshape([-1 if axis == axis_at else 1 for axis in range(len(extent))])
    return factor_of


def noise(key, shape, spread, reach, shards=(), kind=jnp.bfloat16):
    values = spread * jax.random.normal(key, shape, jnp.float32)
    if shards:
        values = values * levels(key, shape, shards, -0.22, 0.18)
    return jnp.clip(values, -reach, reach).astype(kind)


def setup_inputs(seed: int = 0) -> dict:
    keys = jax.random.split(jax.random.key(seed), 8)
    return {
        "tokens": noise(keys[0], (TOKENS, D), 1.0, 6.0, ((0, 32),)),
        "out_grad": noise(keys[1], (TOKENS, D), 0.5, 3.0, ((0, 32),)),
        "expert_ids": draw_expert_ids(jax.random.fold_in(keys[7], 71), 0),
        "route_weights": jnp.clip(jnp.exp(math.log(1.0) - 2.306499 * jax.random.uniform(keys[3], (TOKENS, TOPK), jnp.float32) ** levels(keys[3], (TOKENS, TOPK), ((0, 32),), -0.2, 0.2)), 0.099609375, 1.0).astype(jnp.bfloat16),
        "gate_matrix": noise(keys[4], (D, EXPERTS * FF), D ** -0.5, 0.0625, ((0, 4), (1, 8))),
        "up_matrix": noise(keys[5], (D, EXPERTS * FF), D ** -0.5, 0.0625, ((0, 4), (1, 8))),
        "down_matrix": noise(keys[6], (D, EXPERTS * FF), FF ** -0.5, 0.125, ((0, 4), (1, 8))),
    }


def assignments(expert_ids):
    blocks = expert_ids.shape[0] // TOK_DEV
    flat_ids = expert_ids.reshape(blocks, TOK_DEV * TOPK)
    window = (flat_ids % STRIDE) == 0
    expert = jnp.where(window, flat_ids // STRIDE, EXPERTS).astype(jnp.int32)
    column = jnp.arange(EXPERTS, dtype=jnp.int32)
    onehot = (expert[:, :, None] == column[None, None, :]).astype(jnp.int32)
    earlier = jnp.cumsum(onehot, axis=1) - onehot
    slot_index = jnp.sum(earlier * onehot, axis=2)
    kept_entry = window & (slot_index < CAP)
    target = expert * CAP + slot_index
    places = jnp.arange(EXPERTS * CAP, dtype=jnp.int32)
    table = kept_entry[:, :, None] & (target[:, :, None] == places[None, None, :])
    return table.reshape(blocks, TOK_DEV, TOPK, EXPERTS * CAP).astype(jnp.float32)


def widen(values):
    return lax.optimization_barrier(values.astype(jnp.bfloat16)).astype(jnp.float32)


def reference(tokens, out_grad, expert_ids, route_weights, gate_matrix, up_matrix, down_matrix):
    table = assignments(expert_ids)
    blocks = table.shape[0]
    select = jnp.sum(table, axis=2)
    select_half = select.astype(jnp.bfloat16)

    def dispatch_block(arguments):
        choose, block_in, block_grad = arguments
        first = jnp.dot(choose.T, block_in, preferred_element_type=jnp.float32).astype(jnp.bfloat16)
        second = jnp.dot(choose.T, block_grad, preferred_element_type=jnp.float32).astype(jnp.bfloat16)
        return first, second

    slot_in, slot_grad = lax.map(dispatch_block, (select_half, tokens.reshape(blocks, TOK_DEV, D), out_grad.reshape(blocks, TOK_DEV, D)))
    slot_gate = jnp.einsum("btks,btk->bs", table, route_weights.astype(jnp.float32).reshape(blocks, TOK_DEV, TOPK), precision=lax.Precision.HIGHEST).astype(jnp.bfloat16)

    def arrange(values):
        shaped = values.reshape((N_DP, N_EP, EXPERTS, CAP) + values.shape[2:])
        moved = jnp.moveaxis(shaped, 2, 0)
        return moved.reshape((EXPERTS, N_DP, N_EP * CAP) + values.shape[2:])

    def unarrange(values):
        shaped = values.reshape((EXPERTS, N_DP, N_EP, CAP) + values.shape[3:])
        moved = jnp.moveaxis(shaped, 0, 2)
        return moved.reshape((blocks, EXPERTS * CAP) + values.shape[3:])

    def expert_backward(arguments):
        rows_in, rows_grad, rows_gate, expert = arguments
        begin = (expert * FF).astype(jnp.int32)
        gate_cols = lax.dynamic_slice_in_dim(gate_matrix, begin, FF, 1)
        up_cols = lax.dynamic_slice_in_dim(up_matrix, begin, FF, 1)
        down_cols = lax.dynamic_slice_in_dim(down_matrix, begin, FF, 1)

        def one_group(total, group_arguments):
            group_in, group_grad, group_gate = group_arguments
            row_count = group_in.shape[0]
            gate_pre = jnp.dot(group_in, gate_cols, preferred_element_type=jnp.float32)
            up_pre = jnp.dot(group_in, up_cols, preferred_element_type=jnp.float32)
            projected = jnp.dot(group_grad, down_cols, preferred_element_type=jnp.float32)
            sigmoid = jax.nn.sigmoid(gate_pre)
            swished = gate_pre * sigmoid
            hidden = widen(swished * up_pre)
            slice_sums = jnp.sum((hidden * projected).reshape(row_count, SLICES, HID_DEV), axis=2)
            route_part = jnp.sum(widen(slice_sums), axis=1)
            scaling = group_gate.astype(jnp.float32)[:, None]
            grad_hidden = scaling * projected
            gate_delta = (grad_hidden * up_pre * sigmoid * (1.0 + gate_pre * (1.0 - sigmoid))).astype(jnp.bfloat16)
            up_delta = (grad_hidden * swished).astype(jnp.bfloat16)
            scaled = (scaling * hidden).astype(jnp.bfloat16)
            partial_value = jnp.zeros((row_count, D), jnp.float32)
            for piece in range(SLICES):
                low = piece * HID_DEV
                high = low + HID_DEV
                term = jnp.dot(gate_delta[:, low:high], gate_cols[:, low:high].T, preferred_element_type=jnp.float32)
                term = term + jnp.dot(up_delta[:, low:high], up_cols[:, low:high].T, preferred_element_type=jnp.float32)
                partial_value = partial_value + widen(term)
            grads = jnp.concatenate([
                jnp.dot(group_in.T, gate_delta, preferred_element_type=jnp.float32),
                jnp.dot(group_in.T, up_delta, preferred_element_type=jnp.float32),
                jnp.dot(group_grad.T, scaled, preferred_element_type=jnp.float32)], axis=1)
            total = total + widen(grads)
            return total, (partial_value, route_part)

        start_total = jnp.zeros((D, 3 * FF), jnp.float32)
        total, outputs = lax.scan(one_group, start_total, (rows_in, rows_grad, rows_gate))
        return total.astype(jnp.bfloat16), outputs[0], outputs[1]

    totals, partials, route_parts = lax.map(expert_backward, (arrange(slot_in), arrange(slot_grad), arrange(slot_gate), jnp.arange(EXPERTS, dtype=jnp.int32)))
    slot_partial = unarrange(partials)
    slot_route = unarrange(route_parts)

    def combine_block(arguments):
        choose, values = arguments
        return jnp.dot(choose, values, precision=lax.Precision.HIGHEST).astype(jnp.bfloat16)

    input_gradient = lax.map(combine_block, (select, slot_partial)).reshape(blocks * TOK_DEV, D)
    route_gradient = jnp.einsum("btks,bs->btk", table, slot_route, precision=lax.Precision.HIGHEST).reshape(blocks * TOK_DEV, TOPK)
    gate_gradient = jnp.moveaxis(totals[:, :, :FF], 0, 1).reshape(D, EXPERTS * FF)
    up_gradient = jnp.moveaxis(totals[:, :, FF:2 * FF], 0, 1).reshape(D, EXPERTS * FF)
    down_gradient = jnp.moveaxis(totals[:, :, 2 * FF:], 0, 1).reshape(D, EXPERTS * FF)
    return (input_gradient, route_gradient, gate_gradient, up_gradient, down_gradient)
```

```python
import functools
import jax
import jax.numpy as jnp
from jax import lax
from jax.experimental import pallas as pl
from jax.experimental.pallas import tpu as pltpu
from jax.sharding import PartitionSpec as P

ROUTED = 256
TOPK = 8
SLICES = 8
CAP = 8
LANES = 128
PAIR = 2 * CAP
VMEM_BYTES = 56 * 1024 * 1024
BF = jnp.bfloat16
F32 = jnp.float32
MESH = pl.DeviceIdType.MESH


def kernel(
    n_dp, n_ep,
    tok_hbm, grad_hbm, ids_hbm, rw_hbm, a_hbm, b_hbm, c_hbm,
    ret, sel_ref, ga, gb, gc,
    ids_buf, rw_buf, tokbuf, gradbuf, wab, wc, send1, shard, xs, ys,
    psx, psy, asx, arx, asy, ary, deltas, hiddens, rp, r1recv, r2send,
    in_sem, id_sem, w_sem, s1s, s1r, sus, sds, slr, sfs, sfr, ars, arr, r1s, r1r, r2s, r2r,
):
    experts = n_ep // SLICES
    stride = ROUTED // experts
    places = experts * CAP
    n_hi = n_ep // 2
    per = SLICES // 2
    n_pair = n_dp // 2
    rows, width = tok_hbm.shape
    lw, hid = a_hbm.shape
    nb = n_dp.bit_length() - 1
    chunk = 2 * n_dp * CAP
    half = n_dp * CAP
    g = lax.axis_index("dp")
    e = lax.axis_index("ep")
    hi, lo = e // 2, e % 2
    other = hi * 2 + (1 - lo)
    mine_w = hi // per
    pos = hi % per

    def rc(src, dst, ss, rs, **where):
        return pltpu.make_async_remote_copy(
            src_ref=src, dst_ref=dst, send_sem=ss, recv_sem=rs,
            device_id=where, device_id_type=MESH)

    def flip(j):
        gp = g
        for b in range(nb):
            if j >> b & 1:
                gp = gp + (1 - 2 * ((g // (1 << b)) % 2)) * (1 << b)
        return gp

    def line(i):
        return lax.rem(mine_w + i, experts)

    def place(v):
        return (v * per + pos) * 2 + lo

    id_copies = [
        pltpu.make_async_copy(ids_hbm, ids_buf, id_sem.at[0]),
        pltpu.make_async_copy(rw_hbm, rw_buf, id_sem.at[1]),
    ]
    for c in id_copies:
        c.start()
    order = list(range(1, n_dp)) + [0]
    loads = []
    for q, (src, buf) in enumerate(((tok_hbm, tokbuf), (grad_hbm, gradbuf))):
        for j in order:
            gp = flip(j)
            ds = pl.ds(pl.multiple_of(gp * lw, LANES), lw)
            c = pltpu.make_async_copy(src.at[:, ds], buf.at[j], in_sem.at[q, j])
            c.start()
            loads.append((q, j, gp, buf, c))
    wloads = [
        pltpu.make_async_copy(a_hbm, wab.at[:, pl.ds(0, hid)], w_sem.at[0]),
        pltpu.make_async_copy(b_hbm, wab.at[:, pl.ds(hid, hid)], w_sem.at[1]),
        pltpu.make_async_copy(c_hbm, wc, w_sem.at[2]),
    ]

    barrier = pltpu.get_barrier_semaphore()
    peers = 0
    for i in range(experts):
        for j in range(n_dp):
            if i or j:
                pl.semaphore_signal(
                    barrier, inc=1, device_id={"dp": flip(j), "ep": place(line(i))}, device_id_type=MESH)
                peers += 1
    pl.semaphore_signal(barrier, inc=1, device_id={"ep": other}, device_id_type=MESH)
    peers += 1

    @pl.when(pos > 0)
    def _():
        pl.semaphore_signal(barrier, inc=1, device_id={"ep": e - 2}, device_id_type=MESH)

    @pl.when(pos < per - 1)
    def _():
        pl.semaphore_signal(barrier, inc=1, device_id={"ep": e + 2}, device_id_type=MESH)

    for c in id_copies:
        c.wait()
    pad = jnp.zeros((LANES - TOPK, rows), F32)
    ids = jnp.concatenate([ids_buf[...].astype(F32), pad], axis=0).T
    rw = jnp.concatenate([rw_buf[...].astype(F32), pad], axis=0).T
    lane = lax.broadcasted_iota(jnp.int32, (rows, LANES), 1)
    wanted = jnp.where(lane < places, (lane // CAP) * stride, -1).astype(F32)
    hits = jnp.zeros((rows, LANES), F32)
    wts = jnp.zeros((rows, LANES), F32)
    for k in range(TOPK):
        m = ids[:, k:k + 1] == wanted
        hits = hits + jnp.where(m, 1.0, 0.0)
        wts = wts + jnp.where(m, rw[:, k:k + 1], 0.0)
    tr = lax.broadcasted_iota(jnp.int32, (rows, rows), 0)
    tc = lax.broadcasted_iota(jnp.int32, (rows, rows), 1)
    lower = jnp.where(tc < tr, 1.0, 0.0).astype(BF)
    slot = jnp.dot(lower, hits.astype(BF), preferred_element_type=F32)
    sel = jnp.where(slot == (lane % CAP).astype(F32), hits, 0.0)
    sel_ref[...] = sel
    picks = (sel.T[:places].astype(BF), (sel * wts).T[:places].astype(BF))

    pieces = (pl.ds(0, lw), pl.ds(lw, lw))

    def to_shard(j, i, q, gp):
        v = line(i)
        return rc(send1.at[j, v, :, pieces[q]], shard.at[mine_w, g, :, pieces[q]],
                  s1s.at[q, j, i], s1r.at[q, mine_w, g], dp=gp, ep=place(v))

    def shard_in(q, v, src):
        r = shard.at[v, src, :, pieces[q]]
        return rc(r, r, s1r.at[q, v, src], s1r.at[q, v, src], ep=other)

    first = True
    for q, j, gp, buf, c in loads:
        c.wait()
        r = jnp.dot(picks[q], buf[j], preferred_element_type=F32).reshape(experts, CAP, lw).astype(BF)
        send1[j, :, :, q * lw:(q + 1) * lw] = r
        if first:
            pl.semaphore_wait(
                barrier, peers + jnp.where(pos > 0, 1, 0) + jnp.where(pos < per - 1, 1, 0))
            first = False
        for i in range(experts):
            if i or j:
                to_shard(j, i, q, gp).start()
        if j == 0:
            if experts == 1:
                shard[0, g, :, q * lw:(q + 1) * lw] = r[0]
            else:
                shard[mine_w, g, :, q * lw:(q + 1) * lw] = send1[0, mine_w, :, q * lw:(q + 1) * lw]
    for c in wloads:
        c.start()

    def at_order(k):
        m = jnp.where(pos < per - 1 - pos, pos, per - 1 - pos)
        near = jnp.where(k % 2 == 1, pos - (k + 1) // 2, pos + k // 2)
        far = jnp.where(pos < per - 1 - pos, k, per - 1 - k)
        return jnp.where(k <= 2 * m, near, far)

    def rows_at(h, l, c):
        return pl.ds(pl.multiple_of(((h * 2 + l) * n_dp + 2 * c) * CAP, PAIR), PAIR)

    def piece(q, h, l, c):
        return (ys if q else xs).at[rows_at(h, l, c), :]

    def pair_at(ci):
        return lax.rem(g // 2 + ci, n_pair)

    def link(h, q, c, up):
        k = q * n_pair + c
        r = piece(q, h, lo, c)
        to = e + 2 - 4 * up
        return rc(r, r, (sds if up else sus).at[h, k], slr.at[h, k], ep=to)

    def link_in(h, q, c):
        k = q * n_pair + c
        r = piece(q, h, lo, c)
        return rc(r, r, slr.at[h, k], slr.at[h, k], ep=other)

    def fwd(h, q, c):
        k = q * n_pair + c
        r = piece(q, h, lo, c)
        return rc(r, r, sfs.at[h, k], sfr.at[h, k], ep=other)

    def fwd_in(h, q, c):
        k = q * n_pair + c
        r = piece(q, h, 1 - lo, c)
        return rc(r, r, sfr.at[h, k], sfr.at[h, k], ep=other)

    def onward(h, q, c, up, wait):
        @pl.when((pos > 0) if up else (pos < per - 1))
        def _():
            d = link(h, q, c, up)
            d.wait_send() if wait else d.start()

    for ci in range(n_pair):
        c = pair_at(ci)
        for q in range(2):
            for i in range(experts):
                v = line(i)
                h = v * per + pos
                for b in range(2):
                    src = flip(b) if ci == 0 else 2 * c + b
                    if not (ci == 0 and b == 0 and i == 0):
                        shard_in(q, v, src).wait_recv()
                both = shard[v, pl.ds(2 * c, 2), :, q * lw:(q + 1) * lw]
                (ys if q else xs)[rows_at(h, lo, c), :] = both.astype(F32).reshape(PAIR, lw).astype(BF)
                onward(h, q, c, 0, False)
                onward(h, q, c, 1, False)
                fwd(h, q, c).start()
    for c in wloads:
        c.wait()

    def ar(b, h, part):
        bit = 1 << b
        peer = g + (1 - 2 * ((g // bit) % 2)) * bit
        src, dst = ((asx, arx), (asy, ary))[part]
        return rc(src.at[b, h], dst.at[b, h], ars.at[b, h, part], arr.at[b, h, part], dp=peer)

    def at_chunk(h):
        return pl.ds(pl.multiple_of(h * chunk, PAIR), chunk)

    def r1(h):
        return rc(rp.at[h, 1 - lo], r1recv.at[h], r1s.at[h], r1r.at[h], ep=other)

    def chunk_of(t):
        return at_order(t // experts), t % experts

    def index_of(t):
        p, v = chunk_of(t)
        return v * per + p

    def gather_step(s):
        def one(v, carry):
            for q in range(2):
                for ci in range(n_pair):
                    c = pair_at(ci)

                    @pl.when(pos >= s)
                    def _():
                        h = v * per + pos - s
                        link_in(h, q, c).wait_recv()
                        onward(h, q, c, 0, False)
                        fwd(h, q, c).start()

                    @pl.when(pos + s <= per - 1)
                    def _():
                        h = v * per + pos + s
                        link_in(h, q, c).wait_recv()
                        onward(h, q, c, 1, False)
                        fwd(h, q, c).start()
            return carry

        if experts == 1:
            one(0, 0)
        else:
            lax.fori_loop(0, experts, one, 0)

    def project(t):
        h = index_of(t)
        for ci in range(n_pair):
            fwd_in(h, 0, pair_at(ci)).wait_recv()
        p1 = jnp.dot(xs[at_chunk(h), :], wab[...], preferred_element_type=F32)
        psx[h] = p1
        asx[0, h] = p1.astype(BF)
        ar(0, h, 0).start()
        for ci in range(n_pair):
            fwd_in(h, 1, pair_at(ci)).wait_recv()
        p2 = jnp.dot(ys[at_chunk(h), :], wc[...], preferred_element_type=F32)
        psy[h] = p2
        asy[0, h] = p2.astype(BF)
        ar(0, h, 1).start()

    def reduce_step(t, b):
        h = index_of(t)
        for part, (ps, send, recv) in enumerate(((psx, asx, arx), (psy, asy, ary))):
            ar(b, h, part).wait_recv()
            s = ps[h] + recv[b, h].astype(F32)
            ps[h] = s
            send[b + 1, h] = s.astype(BF)
            ar(b + 1, h, part).start()

    def finish(t):
        h = index_of(t)
        ar(nb - 1, h, 0).wait_recv()
        s = psx[h] + arx[nb - 1, h].astype(F32)
        gate_pre, up_pre = s[:, :hid], s[:, hid:]
        sig = 1.0 / (1.0 + jnp.exp(-gate_pre))
        sw = gate_pre * sig
        hidden = (sw * up_pre).astype(BF)
        hiddens[at_chunk(h), :] = hidden
        slope = up_pre * sig * (1.0 + gate_pre * (1.0 - sig))
        ar(nb - 1, h, 1).wait_recv()
        proj = psy[h] + ary[nb - 1, h].astype(F32)
        route = jnp.sum(hidden.astype(F32) * proj, axis=1, keepdims=True)
        d1 = (proj * slope).astype(BF)
        d2 = (proj * sw).astype(BF)
        deltas[at_chunk(h), 0:hid] = d1
        deltas[at_chunk(h), hid:] = d2
        part = lax.dot_general(
            jnp.concatenate([d1, d2], axis=1), wab[...], (((1,), (1,)), ((), ())),
            preferred_element_type=F32)
        rp[h, :, :, 0:lw] = part.reshape(2, half, lw).astype(BF)
        rp[h, :, :, lw:] = jnp.broadcast_to(route, (chunk, LANES)).reshape(2, half, LANES).astype(BF)
        r1(h).start()

    def r2(h, j):
        gp = flip(j)
        return rc(r2send.at[h, gp], ret.at[hi, g], r2s.at[h, j], r2r.at[hi, g], dp=gp, ep=h * 2 + lo)

    def r2_in(h, src):
        r = ret.at[h, src]
        return rc(r, r, r2r.at[h, src], r2r.at[h, src], ep=other)

    def send_back(t):
        h = index_of(t)
        r1(h).wait_recv()
        both = rp[h, lo].astype(F32) + r1recv[h].astype(F32)
        r2send[h] = both.reshape(n_dp, CAP, lw + LANES).astype(BF)
        for j in range(1, n_dp):
            r2(h, j).start()

        @pl.when(h != hi)
        def _():
            r2(h, 0).start()

        @pl.when(h == hi)
        def _():
            ret[hi, g] = r2send[h, g]

    early = n_hi - 2

    def flow(t, carry):
        s = t // experts

        @pl.when((s >= 1) & (s < per) & (t % experts == 0))
        def _():
            gather_step(s)

        for b in range(nb - 1):
            @pl.when((t >= 2 + b) & (t < n_hi + 2 + b))
            def _(b=b):
                reduce_step(t - 2 - b, b)

        @pl.when((t >= nb + 1) & (t < n_hi + nb + 1))
        def _():
            finish(t - nb - 1)

        @pl.when((t >= 1) & (t <= n_hi))
        def _():
            project(t - 1)

        @pl.when((t >= nb + 3) & (t < early + nb + 3))
        def _():
            send_back(t - nb - 3)
        return carry

    lax.fori_loop(1, n_hi + nb + 1, flow, 0)

    tile = 256 if lw % 256 == 0 else 128

    def wgrad(i, carry):
        ds = pl.ds(pl.multiple_of(i * tile, LANES), tile)
        dn = (((0,), (0,)), ((), ()))
        both = lax.dot_general(xs[:, ds], deltas[...], dn, preferred_element_type=F32).astype(BF)
        ga[ds, :] = both[:, :hid]
        gb[ds, :] = both[:, hid:]
        gc[ds, :] = lax.dot_general(ys[:, ds], hiddens[...], dn, preferred_element_type=F32).astype(BF)
        return carry

    lax.fori_loop(0, lw // tile, wgrad, 0)

    def rest(t, carry):
        send_back(t)
        return carry

    lax.fori_loop(early, n_hi, rest, 0)

    def collect(i, carry):
        h = lax.rem(hi + i, n_hi)
        for j in range(1, n_dp):
            r2_in(h, flip(j)).wait_recv()

        @pl.when(i >= 1)
        def _():
            r2_in(h, g).wait_recv()
        return carry

    lax.fori_loop(0, n_hi, collect, 0)

    for q in range(2):
        for j in range(n_dp):
            for i in range(experts):
                if i or j:
                    to_shard(j, i, q, flip(j)).wait_send()

    def drain(i, carry):
        h = lax.rem(hi + i, n_hi)
        p = h % per
        for q in range(2):
            for ci in range(n_pair):
                c = pair_at(ci)
                fwd(h, q, c).wait_send()

                @pl.when(p <= pos)
                def _():
                    onward(h, q, c, 0, True)

                @pl.when(p >= pos)
                def _():
                    onward(h, q, c, 1, True)
        for b in range(nb):
            for part in range(2):
                ar(b, h, part).wait_send()
        r1(h).wait_send()
        for j in range(1, n_dp):
            r2(h, j).wait_send()

        @pl.when(i >= 1)
        def _():
            r2(h, 0).wait_send()
        return carry

    lax.fori_loop(0, n_hi, drain, 0)


def finish_kernel(
    ret, sel_ref, ga, gb, gc, ids_ref, rw_ref, ig_hbm, rg_ref, ga_out, gb_out, gc_out,
    obuf, sem_out, osem,
):
    n_hi, n_dp, _, wide = ret.shape
    per = SLICES // 2
    experts = n_hi // per
    places = experts * CAP
    lw = wide - LANES
    rows = sel_ref.shape[0]
    stride = ROUTED // experts
    outs = [
        pltpu.make_async_copy(src, dst, sem_out.at[i])
        for i, (src, dst) in enumerate(((ga, ga_out), (gb, gb_out), (gc, gc_out)))
    ]
    for c in outs:
        c.start()
    sel = sel_ref[...]
    selP = sel[:, :places].astype(BF)

    def total(j):
        parts = []
        for w in range(experts):
            acc = ret[w * per, j].astype(F32)
            for i in range(1, per):
                acc = acc + ret[w * per + i, j].astype(F32)
            parts.append(acc)
        return jnp.concatenate(parts, axis=0) if experts > 1 else parts[0]

    ocopies = []
    for j in range(n_dp):
        vals = total(j)
        if j == 0:
            route = vals[:, lw:]
        obuf[:, j * lw:(j + 1) * lw] = jnp.dot(
            selP, vals[:, :lw].astype(BF), preferred_element_type=F32).astype(BF)
        ds = pl.ds(j * lw, lw)
        c = pltpu.make_async_copy(obuf.at[:, ds], ig_hbm.at[:, ds], osem.at[j])
        c.start()
        ocopies.append(c)
    route = jnp.concatenate([route, jnp.zeros((LANES - places, LANES), F32)], axis=0).T[0:1]
    terms = sel * route
    pad = jnp.zeros((LANES - TOPK, rows), F32)
    ids = jnp.concatenate([ids_ref[...].astype(F32), pad], axis=0).T
    lane = lax.broadcasted_iota(jnp.int32, (rows, LANES), 1)
    wanted = jnp.where(lane < places, (lane // CAP) * stride, -1).astype(F32)
    rg = jnp.zeros((rows, LANES), F32)
    for k in range(TOPK):
        v = jnp.sum(jnp.where(ids[:, k:k + 1] == wanted, terms, 0.0), axis=1, keepdims=True)
        rg = jnp.where(lane == k, v, rg)
    rg_ref[...] = rg.T[:TOPK] / rw_ref[...].astype(F32)
    for c in outs + ocopies:
        c.wait()


def body(tokens, out_grad, expert_ids, route_weights, gate_matrix, up_matrix, down_matrix):
    n_dp, n_ep = lax.axis_size("dp"), lax.axis_size("ep")
    experts = n_ep // SLICES
    n_hi = n_ep // 2
    n_pair = n_dp // 2
    rows, width = tokens.shape
    lw, hid = gate_matrix.shape
    nb = n_dp.bit_length() - 1
    chunk = 2 * n_dp * CAP
    half = n_dp * CAP
    total = n_hi * chunk
    R = lw + LANES
    K = 2 * n_pair
    V = pltpu.VMEM
    D = lambda *s: pltpu.SemaphoreType.DMA(s)
    anyspec = pl.BlockSpec(memory_space=pl.ANY)
    vspec = pl.BlockSpec(memory_space=pltpu.VMEM)
    ids, rw = expert_ids.T, route_weights.T
    grad = jax.ShapeDtypeStruct((lw, hid), BF)
    ret, sel, ga, gb, gc = pl.pallas_call(
        functools.partial(kernel, n_dp, n_ep),
        out_shape=(
            V((n_hi, n_dp, CAP, R), BF), V((rows, LANES), F32),
            V((lw, hid), BF), V((lw, hid), BF), V((lw, hid), BF),
        ),
        in_specs=[anyspec] * 7,
        out_specs=(vspec,) * 5,
        scratch_shapes=[
            V((TOPK, rows), jnp.int32), V((TOPK, rows), BF),
            V((n_dp, rows, lw), BF), V((n_dp, rows, lw), BF), V((lw, 2 * hid), BF), V((lw, hid), BF),
            V((n_dp, experts, CAP, 2 * lw), BF), V((experts, n_dp, CAP, 2 * lw), BF),
            V((total, lw), BF), V((total, lw), BF),
            V((n_hi, chunk, 2 * hid), F32), V((n_hi, chunk, hid), F32),
            V((nb, n_hi, chunk, 2 * hid), BF), V((nb, n_hi, chunk, 2 * hid), BF),
            V((nb, n_hi, chunk, hid), BF), V((nb, n_hi, chunk, hid), BF),
            V((total, 2 * hid), BF), V((total, hid), BF),
            V((n_hi, 2, half, R), BF), V((n_hi, half, R), BF), V((n_hi, n_dp, CAP, R), BF),
            D(2, n_dp), D(2), D(3), D(2, n_dp, experts), D(2, experts, n_dp),
            D(n_hi, K), D(n_hi, K), D(n_hi, K), D(n_hi, K), D(n_hi, K),
            D(nb, n_hi, 2), D(nb, n_hi, 2), D(n_hi), D(n_hi), D(n_hi, n_dp), D(n_hi, n_dp),
        ],
        compiler_params=pltpu.CompilerParams(
            collective_id=0, has_side_effects=True, vmem_limit_bytes=VMEM_BYTES),
    )(tokens, out_grad, ids, rw, gate_matrix, up_matrix, down_matrix)
    keep = [pltpu.with_memory_space_constraint(a, pltpu.VMEM) for a in (ret, sel, ga, gb, gc)]
    ig, rg, ga, gb, gc = pl.pallas_call(
        finish_kernel,
        out_shape=(
            jax.ShapeDtypeStruct((rows, width), BF),
            jax.ShapeDtypeStruct((TOPK, rows), F32),
            grad, grad, grad,
        ),
        in_specs=[vspec] * 7,
        out_specs=(anyspec, vspec, anyspec, anyspec, anyspec),
        scratch_shapes=[V((rows, width), BF), D(3), D(n_dp)],
        compiler_params=pltpu.CompilerParams(vmem_limit_bytes=16 * 1024 * 1024),
    )(*keep, ids, rw)
    return ig, rg.T, ga, gb, gc


def solution(mesh):
    return jax.shard_map(
        body,
        mesh=mesh,
        in_specs=(
            P(("dp", "ep"), None),
            P(("dp", "ep"), None),
            P(("dp", "ep"), None),
            P(("dp", "ep"), None),
            P("dp", "ep"),
            P("dp", "ep"),
            P("dp", "ep"),
        ),
        out_specs=(
            P(("dp", "ep"), None),
            P(("dp", "ep"), None),
            P("dp", "ep"),
            P("dp", "ep"),
            P("dp", "ep"),
        ),
        check_vma=False,
    )
```

```python
import functools
import jax
import jax.numpy as jnp
from jax import lax
from jax.experimental import pallas as pl
from jax.experimental.pallas import tpu as pltpu
from jax.sharding import PartitionSpec as P

ROUTED = 256
TOPK = 8
SLICES = 8
CAP = 8
LANES = 128
PAIR = 2 * CAP
VMEM_BYTES = 56 * 1024 * 1024
BF = jnp.bfloat16
F32 = jnp.float32
MESH = pl.DeviceIdType.MESH


def kernel(
    n_dp, n_ep,
    tok_hbm, grad_hbm, ids_hbm, rw_hbm, a_hbm, b_hbm, c_hbm,
    ret, rret, sel_ref, ga, gb, gc,
    ids_buf, rw_buf, tokbuf, gradbuf, w3, send1, shard, xs, ys,
    psx, psy, asx, arx, asy, ary, deltas, hiddens, rp, r1recv, r2send, rsend,
    in_sem, id_sem, out_sem, s1r, slr, sfr, arr, r1r,
):
    experts = n_ep // SLICES
    stride = ROUTED // experts
    places = experts * CAP
    n_hi = n_ep // 2
    per = SLICES // 2
    n_pair = n_dp // 2
    rows, width = tok_hbm.shape
    lw, hid = a_hbm.shape
    nb = n_dp.bit_length() - 1
    chunk = 2 * n_dp * CAP
    half = n_dp * CAP
    wab, wc = w3.at[:, pl.ds(0, 2 * hid)], w3.at[:, pl.ds(2 * hid, hid)]
    w_sem, s1s, sus, sds, sfs, asxs, asys, r1s, r2s, r2r, rts, rtr = (out_sem.at[i] for i in range(12))
    g = lax.axis_index("dp")
    e = lax.axis_index("ep")
    hi, lo = e // 2, e % 2
    other = hi * 2 + (1 - lo)
    mine_w = hi // per
    pos = hi % per

    def rc(src, dst, ss, rs, **where):
        return pltpu.make_async_remote_copy(
            src_ref=src, dst_ref=dst, send_sem=ss, recv_sem=rs,
            device_id=where, device_id_type=MESH)

    def flip(j):
        gp = g
        for b in range(nb):
            if j >> b & 1:
                gp = gp + (1 - 2 * ((g // (1 << b)) % 2)) * (1 << b)
        return gp

    def line(i):
        return lax.rem(mine_w + i, experts)

    def place(v):
        return (v * per + pos) * 2 + lo

    id_copies = [
        pltpu.make_async_copy(ids_hbm, ids_buf, id_sem.at[0]),
        pltpu.make_async_copy(rw_hbm, rw_buf, id_sem.at[1]),
    ]
    for c in id_copies:
        c.start()
    order = list(range(1, n_dp)) + [0]
    loads = []
    for q, (src, buf) in enumerate(((tok_hbm, tokbuf), (grad_hbm, gradbuf))):
        for j in order:
            gp = flip(j)
            ds = pl.ds(pl.multiple_of(gp * lw, LANES), lw)
            c = pltpu.make_async_copy(src.at[:, ds], buf.at[j], in_sem.at[q, j])
            if q == 0:
                c.start()
            loads.append((q, j, gp, buf, c))
    wloads = [
        pltpu.make_async_copy(w, w3.at[:, pl.ds(i * hid, hid)], w_sem)
        for i, w in enumerate((a_hbm, b_hbm, c_hbm))
    ]

    barrier = pltpu.get_barrier_semaphore()
    peers = 0
    for i in range(experts):
        for j in range(n_dp):
            if i or j:
                pl.semaphore_signal(
                    barrier, inc=1, device_id={"dp": flip(j), "ep": place(line(i))}, device_id_type=MESH)
                peers += 1
    pl.semaphore_signal(barrier, inc=1, device_id={"ep": other}, device_id_type=MESH)
    peers += 1

    @pl.when(pos > 0)
    def _():
        pl.semaphore_signal(barrier, inc=1, device_id={"ep": e - 2}, device_id_type=MESH)

    @pl.when(pos < per - 1)
    def _():
        pl.semaphore_signal(barrier, inc=1, device_id={"ep": e + 2}, device_id_type=MESH)

    for c in id_copies:
        c.wait()
    for q, j, gp, buf, c in loads:
        if q:
            c.start()
    pad = jnp.zeros((LANES - TOPK, rows), F32)
    ids = jnp.concatenate([ids_buf[...].astype(F32), pad], axis=0).T
    rw = jnp.concatenate([rw_buf[...].astype(F32), pad], axis=0).T
    lane = lax.broadcasted_iota(jnp.int32, (rows, LANES), 1)
    wanted = jnp.where(lane < places, (lane // CAP) * stride, -1).astype(F32)
    hits = jnp.zeros((rows, LANES), F32)
    wts = jnp.zeros((rows, LANES), F32)
    for k in range(TOPK):
        m = ids[:, k:k + 1] == wanted
        hits = hits + jnp.where(m, 1.0, 0.0)
        wts = wts + jnp.where(m, rw[:, k:k + 1], 0.0)
    tr = lax.broadcasted_iota(jnp.int32, (rows, rows), 0)
    tc = lax.broadcasted_iota(jnp.int32, (rows, rows), 1)
    lower = jnp.where(tc < tr, 1.0, 0.0).astype(BF)
    slot = jnp.dot(lower, hits.astype(BF), preferred_element_type=F32)
    sel = jnp.where(slot == (lane % CAP).astype(F32), hits, 0.0)
    sel_ref[...] = sel
    picks = (sel.T[:places].astype(BF), (sel * wts).T[:places].astype(BF))

    pieces = (pl.ds(0, lw), pl.ds(lw, lw))

    def to_shard(j, i, q, gp):
        v = line(i)
        return rc(send1.at[j, v, :, pieces[q]], shard.at[mine_w, g, :, pieces[q]],
                  s1s, s1r.at[q, mine_w, g], dp=gp, ep=place(v))

    def shard_in(q, v, src):
        r = shard.at[v, src, :, pieces[q]]
        return rc(r, r, s1r.at[q, v, src], s1r.at[q, v, src], ep=other)

    first = True
    for q, j, gp, buf, c in loads:
        c.wait()
        r = jnp.dot(picks[q], buf[j], preferred_element_type=F32).reshape(experts, CAP, lw).astype(BF)
        send1[j, :, :, q * lw:(q + 1) * lw] = r
        if first:
            pl.semaphore_wait(
                barrier, peers + jnp.where(pos > 0, 1, 0) + jnp.where(pos < per - 1, 1, 0))
            first = False
        for i in range(experts):
            if i or j:
                to_shard(j, i, q, gp).start()
        if j == 0:
            if experts == 1:
                shard[0, g, :, q * lw:(q + 1) * lw] = r[0]
            else:
                shard[mine_w, g, :, q * lw:(q + 1) * lw] = send1[0, mine_w, :, q * lw:(q + 1) * lw]
    for c in wloads:
        c.start()

    def at_order(k):
        m = jnp.where(pos < per - 1 - pos, pos, per - 1 - pos)
        near = jnp.where(k % 2 == 1, pos - (k + 1) // 2, pos + k // 2)
        far = jnp.where(pos < per - 1 - pos, k, per - 1 - k)
        return jnp.where(k <= 2 * m, near, far)

    def rows_at(h, l, c):
        return pl.ds(pl.multiple_of(((h * 2 + l) * n_dp + 2 * c) * CAP, PAIR), PAIR)

    def piece(q, h, l, c):
        return (ys if q else xs).at[rows_at(h, l, c), :]

    def pair_at(ci):
        return lax.rem(g // 2 + ci, n_pair)

    def link(h, q, c, up):
        k = q * n_pair + c
        r = piece(q, h, lo, c)
        to = e + 2 - 4 * up
        return rc(r, r, sds if up else sus, slr.at[h, k], ep=to)

    def link_in(h, q, c):
        k = q * n_pair + c
        r = piece(q, h, lo, c)
        return rc(r, r, slr.at[h, k], slr.at[h, k], ep=other)

    def fwd(h, q, c):
        k = q * n_pair + c
        r = piece(q, h, lo, c)
        return rc(r, r, sfs, sfr.at[h, k], ep=other)

    def cross(h, q, c, up):
        k = q * n_pair + c
        r = piece(q, h, 1 - lo, c)
        return rc(r, r, sds if up else sus, sfr.at[h, k], ep=e + 2 - 4 * up)

    def fwd_in(h, q, c):
        k = q * n_pair + c
        r = piece(q, h, 1 - lo, c)
        return rc(r, r, sfr.at[h, k], sfr.at[h, k], ep=other)

    def onward(h, q, c, up):
        @pl.when((pos > 0) if up else (pos < per - 1))
        def _():
            link(h, q, c, up).start()

    inner = (pos > 0) & (pos < per - 1)

    for ci in range(n_pair):
        c = pair_at(ci)
        for q in range(2):
            for i in range(experts):
                v = line(i)
                h = v * per + pos
                for b in range(2):
                    src = flip(b) if ci == 0 else 2 * c + b
                    if not (ci == 0 and b == 0 and i == 0):
                        shard_in(q, v, src).wait_recv()
                both = shard[v, pl.ds(2 * c, 2), :, q * lw:(q + 1) * lw]
                (ys if q else xs)[rows_at(h, lo, c), :] = both.astype(F32).reshape(PAIR, lw).astype(BF)
                onward(h, q, c, 0)
                onward(h, q, c, 1)
                fwd(h, q, c).start()
    pltpu.make_async_copy(w3, w3, w_sem).wait()

    def ar(b, h, part):
        bit = 1 << b
        peer = g + (1 - 2 * ((g // bit) % 2)) * bit
        src, dst = ((asx, arx), (asy, ary))[part]
        return rc(src.at[b, h], dst.at[b, h], (asxs, asys)[part], arr.at[b, h, part], dp=peer)

    def at_chunk(h):
        return pl.ds(pl.multiple_of(h * chunk, PAIR), chunk)

    def r1(h):
        return rc(rp.at[h, 1 - lo], r1recv.at[h], r1s, r1r.at[h], ep=other)

    def over(stage):
        if experts == 1:
            stage(0)
        else:
            lax.fori_loop(0, experts, lambda v, carry: (stage(v), carry)[1], 0)

    def gather_step(s, v):
        for q in range(2):
            for ci in range(n_pair):
                c = pair_at(ci)
                if s == 1:
                    @pl.when(jnp.logical_not(inner))
                    def _():
                        h = v * per + pos
                        fwd_in(h, q, c).wait_recv()
                        for up in range(2):
                            @pl.when((pos > 0) if up else (pos == 0))
                            def _():
                                cross(h, q, c, up).start()

                for up in range(2):
                    p = pos + s if up else pos - s

                    @pl.when((p <= per - 1) if up else (p >= 0))
                    def _():
                        h = v * per + p
                        link_in(h, q, c).wait_recv()
                        onward(h, q, c, up)
                        if s == 1:
                            @pl.when(jnp.logical_not(inner & ((p == 0) | (p == per - 1))))
                            def _():
                                fwd(h, q, c).start()
                        elif s == 2 or q == 0:
                            fwd(h, q, c).start()

    def cross_far(v):
        for ci in range(n_pair):
            c = pair_at(ci)

            @pl.when(inner)
            def _():
                h = v * per + at_order(per - 1)
                fwd_in(h, 1, c).wait_recv()
                for up in range(2):
                    @pl.when((pos < per // 2) if up else (pos >= per // 2))
                    def _():
                        cross(h, 1, c, up).start()

    def project(k, v):
        h = v * per + at_order(k)

        def arrived(q):
            def wait():
                for ci in range(n_pair):
                    fwd_in(h, q, pair_at(ci)).wait_recv()

            if k == 0:
                pl.when(inner)(wait)
            elif k == per - 1 and q:
                pl.when(jnp.logical_not(inner))(wait)
            else:
                wait()

        arrived(0)
        p1 = jnp.dot(xs[at_chunk(h), :], wab[...], preferred_element_type=F32)
        psx[h] = p1
        asx[0, h] = p1.astype(BF)
        ar(0, h, 0).start()
        arrived(1)
        p2 = jnp.dot(ys[at_chunk(h), :], wc[...], preferred_element_type=F32)
        psy[h] = p2
        asy[0, h] = p2.astype(BF)
        ar(0, h, 1).start()

    def reduce_step(k, b, v):
        h = v * per + at_order(k)
        for part, (ps, send, recv) in enumerate(((psx, asx, arx), (psy, asy, ary))):
            ar(b, h, part).wait_recv()
            s = ps[h] + recv[b, h].astype(F32)
            ps[h] = s
            send[b + 1, h] = s.astype(BF)
            ar(b + 1, h, part).start()

    def finish(k, v):
        h = v * per + at_order(k)
        ar(nb - 1, h, 0).wait_recv()
        s = psx[h] + arx[nb - 1, h].astype(F32)
        gate_pre, up_pre = s[:, :hid], s[:, hid:]
        sig = 1.0 / (1.0 + jnp.exp(-gate_pre))
        sw = gate_pre * sig
        hidden = (sw * up_pre).astype(BF)
        hiddens[at_chunk(h), :] = hidden
        slope = up_pre * sig * (1.0 + gate_pre * (1.0 - sig))
        ar(nb - 1, h, 1).wait_recv()
        proj = psy[h] + ary[nb - 1, h].astype(F32)
        route = jnp.sum(hidden.astype(F32) * proj, axis=1, keepdims=True)
        d1 = (proj * slope).astype(BF)
        d2 = (proj * sw).astype(BF)
        deltas[at_chunk(h), 0:hid] = d1
        deltas[at_chunk(h), hid:] = d2
        part = lax.dot_general(
            jnp.concatenate([d1, d2], axis=1), wab[...], (((1,), (1,)), ((), ())),
            preferred_element_type=F32)
        rp[h] = part.reshape(2, half, lw).astype(BF)
        rsend[h] = jnp.broadcast_to(route, (chunk, LANES)).reshape(2, n_dp, CAP, LANES).astype(BF)
        for l in range(2):
            @pl.when(h * 2 + l != e)
            def _():
                rc(rsend.at[h, l, g], rret.at[e], rts, rtr, ep=h * 2 + l).start()

            @pl.when(h * 2 + l == e)
            def _():
                rret[e] = rsend[h, l, g]

    def r2(h, j):
        gp = flip(j)
        return rc(r2send.at[h, gp], ret.at[hi * n_dp + g], r2s, r2r, dp=gp, ep=h * 2 + lo)

    def send_back(k, v):
        h = v * per + at_order(k)
        r1(h).wait_recv()
        both = rp[h, lo].astype(F32) + r1recv[h].astype(F32)
        r2send[h] = both.reshape(n_dp, CAP, lw).astype(BF)
        for j in range(1, n_dp):
            r2(h, j).start()

        @pl.when(h != hi)
        def _():
            r2(h, 0).start()

        @pl.when(h == hi)
        def _():
            ret[hi * n_dp + g] = r2send[h, g]

    def G(s):
        over(functools.partial(gather_step, s))

    def P(k):
        over(functools.partial(project, k))

    def A(k):
        for b in range(nb - 1):
            over(functools.partial(reduce_step, k, b))

    def F(k):
        over(functools.partial(finish, k))

    def S(k):
        over(lambda v: r1(v * per + at_order(k)).start())

    def R(k):
        over(functools.partial(send_back, k))

    G(1)
    P(0)
    A(0)
    G(2)
    P(1)
    A(1)
    F(0)
    G(3)
    P(2)
    over(cross_far)
    A(2)
    F(1)
    S(1)
    S(0)
    P(3)
    A(3)
    F(2)
    S(2)
    R(1)
    F(3)
    S(3)
    R(0)
    R(2)
    R(3)

    tile = 256 if lw % 256 == 0 else 128

    def wgrad(i, carry):
        ds = pl.ds(pl.multiple_of(i * tile, LANES), tile)
        dn = (((0,), (0,)), ((), ()))
        both = lax.dot_general(xs[:, ds], deltas[...], dn, preferred_element_type=F32).astype(BF)
        ga[ds, :] = both[:, :hid]
        gb[ds, :] = both[:, hid:]
        gc[ds, :] = lax.dot_general(ys[:, ds], hiddens[...], dn, preferred_element_type=F32).astype(BF)
        return carry

    lax.fori_loop(0, lw // tile, wgrad, 0)

    def settle(ref, sem):
        pltpu.make_async_copy(ref, ref, sem).wait()

    back, routes = ret.at[pl.ds(0, n_hi * n_dp - 1)], rret.at[pl.ds(0, n_ep - 1)]
    settle(back, r2r)
    settle(routes, rtr)
    settle(back, r2s)
    settle(routes, rts)
    settle(r1recv, r1s)
    settle(asx, asxs)
    settle(asy, asys)
    settle(xs.at[pl.ds(0, PAIR * (n_dp * experts - 1)), :], s1s)
    K = 2 * n_pair
    for at in range(per):
        ends = at in (0, per - 1)
        crossing = {0: K, per - 2: n_pair}
        down = per - 1 - at
        sent = (
            (sus, (at + 1) * K + crossing.get(at, 0) if down else 0),
            (sds, (down + 1) * K + crossing.get(down, 0) if at else 0),
            (sfs, (per - 1) * K + (n_pair if ends else 0)),
        )

        @pl.when(pos == at)
        def _(sent=sent):
            for sem, count in sent:
                if count:
                    settle(xs.at[pl.ds(0, PAIR * count * experts), :], sem)


def finish_kernel(
    ret, rret, sel_ref, ga, gb, gc, ids_ref, rw_ref, ig_hbm, rg_ref, ga_out, gb_out, gc_out,
    obuf, sem_out, osem,
):
    per = SLICES // 2
    experts = rret.shape[0] // SLICES
    n_dp = ret.shape[0] // (experts * per)
    places = experts * CAP
    lw = ret.shape[2]
    rows = sel_ref.shape[0]
    stride = ROUTED // experts
    outs = [
        pltpu.make_async_copy(src, dst, sem_out.at[i])
        for i, (src, dst) in enumerate(((ga, ga_out), (gb, gb_out), (gc, gc_out)))
    ]
    for c in outs:
        c.start()
    sel = sel_ref[...]
    selP = sel[:, :places].astype(BF)

    def total(ref, base, step, count):
        parts = []
        for w in range(experts):
            acc = ref[w * count * step + base].astype(F32)
            for i in range(1, count):
                acc = acc + ref[(w * count + i) * step + base].astype(F32)
            parts.append(acc)
        return jnp.concatenate(parts, axis=0) if experts > 1 else parts[0]

    ocopies = []
    for j in range(n_dp):
        obuf[:, j * lw:(j + 1) * lw] = jnp.dot(
            selP, total(ret, j, n_dp, per).astype(BF), preferred_element_type=F32).astype(BF)
        ds = pl.ds(j * lw, lw)
        c = pltpu.make_async_copy(obuf.at[:, ds], ig_hbm.at[:, ds], osem.at[j])
        c.start()
        ocopies.append(c)
    route = total(rret, 0, 1, SLICES)
    route = jnp.concatenate([route, jnp.zeros((LANES - places, LANES), F32)], axis=0).T[0:1]
    terms = sel * route
    pad = jnp.zeros((LANES - TOPK, rows), F32)
    ids = jnp.concatenate([ids_ref[...].astype(F32), pad], axis=0).T
    lane = lax.broadcasted_iota(jnp.int32, (rows, LANES), 1)
    wanted = jnp.where(lane < places, (lane // CAP) * stride, -1).astype(F32)
    rg = jnp.zeros((rows, LANES), F32)
    for k in range(TOPK):
        v = jnp.sum(jnp.where(ids[:, k:k + 1] == wanted, terms, 0.0), axis=1, keepdims=True)
        rg = jnp.where(lane == k, v, rg)
    rg_ref[...] = rg.T[:TOPK] / rw_ref[...].astype(F32)
    for c in outs + ocopies:
        c.wait()


def body(tokens, out_grad, expert_ids, route_weights, gate_matrix, up_matrix, down_matrix):
    n_dp, n_ep = lax.axis_size("dp"), lax.axis_size("ep")
    experts = n_ep // SLICES
    n_hi = n_ep // 2
    n_pair = n_dp // 2
    rows, width = tokens.shape
    lw, hid = gate_matrix.shape
    nb = n_dp.bit_length() - 1
    chunk = 2 * n_dp * CAP
    half = n_dp * CAP
    total = n_hi * chunk
    K = 2 * n_pair
    V = pltpu.VMEM
    D = lambda *s: pltpu.SemaphoreType.DMA(s)
    anyspec = pl.BlockSpec(memory_space=pl.ANY)
    vspec = pl.BlockSpec(memory_space=pltpu.VMEM)
    ids, rw = expert_ids.T, route_weights.T
    grad = jax.ShapeDtypeStruct((lw, hid), BF)
    kept = pl.pallas_call(
        functools.partial(kernel, n_dp, n_ep),
        out_shape=(
            V((n_hi * n_dp, CAP, lw), BF), V((n_ep, CAP, LANES), BF), V((rows, LANES), F32),
            V((lw, hid), BF), V((lw, hid), BF), V((lw, hid), BF),
        ),
        in_specs=[anyspec] * 7,
        out_specs=(vspec,) * 6,
        scratch_shapes=[
            V((TOPK, rows), jnp.int32), V((TOPK, rows), BF),
            V((n_dp, rows, lw), BF), V((n_dp, rows, lw), BF), V((lw, 3 * hid), BF),
            V((n_dp, experts, CAP, 2 * lw), BF), V((experts, n_dp, CAP, 2 * lw), BF),
            V((total, lw), BF), V((total, lw), BF),
            V((n_hi, chunk, 2 * hid), F32), V((n_hi, chunk, hid), F32),
            V((nb, n_hi, chunk, 2 * hid), BF), V((nb, n_hi, chunk, 2 * hid), BF),
            V((nb, n_hi, chunk, hid), BF), V((nb, n_hi, chunk, hid), BF),
            V((total, 2 * hid), BF), V((total, hid), BF),
            V((n_hi, 2, half, lw), BF), V((n_hi, half, lw), BF), V((n_hi, n_dp, CAP, lw), BF),
            V((n_hi, 2, n_dp, CAP, LANES), BF),
            D(2, n_dp), D(2), D(12), D(2, experts, n_dp), D(n_hi, K), D(n_hi, K), D(nb, n_hi, 2), D(n_hi),
        ],
        compiler_params=pltpu.CompilerParams(
            collective_id=0, has_side_effects=True, vmem_limit_bytes=VMEM_BYTES),
    )(tokens, out_grad, ids, rw, gate_matrix, up_matrix, down_matrix)
    kept = [pltpu.with_memory_space_constraint(a, pltpu.VMEM) for a in kept]
    ig, rg, ga, gb, gc = pl.pallas_call(
        finish_kernel,
        out_shape=(
            jax.ShapeDtypeStruct((rows, width), BF),
            jax.ShapeDtypeStruct((TOPK, rows), F32),
            grad, grad, grad,
        ),
        in_specs=[vspec] * 8,
        out_specs=(anyspec, vspec, anyspec, anyspec, anyspec),
        scratch_shapes=[V((rows, width), BF), D(3), D(n_dp)],
        compiler_params=pltpu.CompilerParams(vmem_limit_bytes=16 * 1024 * 1024),
    )(*kept, ids, rw)
    return ig, rg.T, ga, gb, gc


def solution(mesh):
    return jax.shard_map(
        body,
        mesh=mesh,
        in_specs=(
            P(("dp", "ep"), None),
            P(("dp", "ep"), None),
            P(("dp", "ep"), None),
            P(("dp", "ep"), None),
            P("dp", "ep"),
            P("dp", "ep"),
            P("dp", "ep"),
        ),
        out_specs=(
            P(("dp", "ep"), None),
            P(("dp", "ep"), None),
            P("dp", "ep"),
            P("dp", "ep"),
            P("dp", "ep"),
        ),
        check_vma=False,
    )
```

```python
import functools
import jax
import jax.numpy as jnp
from jax import lax
from jax.experimental import pallas as pl
from jax.experimental.pallas import tpu as pltpu
from jax.sharding import PartitionSpec as P

ROUTED = 256
TOPK = 8
SLICES = 8
CAP = 8
LANES = 128
PAIR = 2 * CAP
VMEM_BYTES = 56 * 1024 * 1024
BF = jnp.bfloat16
F32 = jnp.float32
MESH = pl.DeviceIdType.MESH


def kernel(
    n_dp, n_ep,
    tok_hbm, grad_hbm, ids_hbm, rw_hbm, a_hbm, b_hbm, c_hbm,
    ret, rret, sel_ref, ga, gb, gc,
    ids_buf, rw_buf, tokbuf, gradbuf, w3, send1, shard, xs, ys,
    psx, psy, asx, arx, asy, ary, deltas, hiddens, rp, r1recv, r2send, rsend,
    in_sem, id_sem, out_sem, s1r, slr, sfr, arr, r1r,
):
    experts = n_ep // SLICES
    stride = ROUTED // experts
    places = experts * CAP
    n_hi = n_ep // 2
    per = SLICES // 2
    n_pair = n_dp // 2
    rows, width = tok_hbm.shape
    lw, hid = a_hbm.shape
    nb = n_dp.bit_length() - 1
    chunk = 2 * n_dp * CAP
    half = n_dp * CAP
    wab, wc = w3.at[:, pl.ds(0, 2 * hid)], w3.at[:, pl.ds(2 * hid, hid)]
    w_sem, s1s, sus, sds, sfs, asxs, asys, r1s, r2s, r2r, rts, rtr = (out_sem.at[i] for i in range(12))
    g = lax.axis_index("dp")
    e = lax.axis_index("ep")
    hi, lo = e // 2, e % 2
    other = hi * 2 + (1 - lo)
    mine_w = hi // per
    pos = hi % per

    def rc(src, dst, ss, rs, **where):
        return pltpu.make_async_remote_copy(
            src_ref=src, dst_ref=dst, send_sem=ss, recv_sem=rs,
            device_id=where, device_id_type=MESH)

    def flip(j):
        gp = g
        for b in range(nb):
            if j >> b & 1:
                gp = gp + (1 - 2 * ((g // (1 << b)) % 2)) * (1 << b)
        return gp

    def line(i):
        return lax.rem(mine_w + i, experts)

    def place(v):
        return (v * per + pos) * 2 + lo

    id_copies = [
        pltpu.make_async_copy(ids_hbm, ids_buf, id_sem.at[0]),
        pltpu.make_async_copy(rw_hbm, rw_buf, id_sem.at[1]),
    ]
    for c in id_copies:
        c.start()
    order = list(range(1, n_dp)) + [0]
    loads = []
    for q, (src, buf) in enumerate(((tok_hbm, tokbuf), (grad_hbm, gradbuf))):
        for j in order:
            gp = flip(j)
            ds = pl.ds(pl.multiple_of(gp * lw, LANES), lw)
            c = pltpu.make_async_copy(src.at[:, ds], buf.at[j], in_sem.at[q, j])
            if q == 0:
                c.start()
            loads.append((q, j, gp, buf, c))
    wloads = [
        pltpu.make_async_copy(w, w3.at[:, pl.ds(i * hid, hid)], w_sem)
        for i, w in enumerate((a_hbm, b_hbm, c_hbm))
    ]

    barrier = pltpu.get_barrier_semaphore()
    peers = 0
    for i in range(experts):
        for j in range(n_dp):
            if i or j:
                pl.semaphore_signal(
                    barrier, inc=1, device_id={"dp": flip(j), "ep": place(line(i))}, device_id_type=MESH)
                peers += 1
    pl.semaphore_signal(barrier, inc=1, device_id={"ep": other}, device_id_type=MESH)
    peers += 1

    @pl.when(pos > 0)
    def _():
        pl.semaphore_signal(barrier, inc=1, device_id={"ep": e - 2}, device_id_type=MESH)

    @pl.when(pos < per - 1)
    def _():
        pl.semaphore_signal(barrier, inc=1, device_id={"ep": e + 2}, device_id_type=MESH)

    for c in id_copies:
        c.wait()
    for q, j, gp, buf, c in loads:
        if q:
            c.start()
    ids, rw = ids_buf[...], rw_buf[...].astype(F32)
    spread = lambda a: jnp.broadcast_to(jnp.sum(a, axis=0, keepdims=True), (CAP, rows))
    hits, wts = [], []
    for w in range(experts):
        m = ids == w * stride
        hits.append(spread(jnp.where(m, 1.0, 0.0)))
        wts.append(spread(jnp.where(m, rw, 0.0)))
    hits = jnp.concatenate(hits, axis=0) if experts > 1 else hits[0]
    wts = jnp.concatenate(wts, axis=0) if experts > 1 else wts[0]
    tr = lax.broadcasted_iota(jnp.int32, (rows, rows), 0)
    tc = lax.broadcasted_iota(jnp.int32, (rows, rows), 1)
    before = jnp.where(tr < tc, 1.0, 0.0).astype(BF)
    slot = jnp.dot(hits.astype(BF), before, preferred_element_type=F32)
    place_in = lax.broadcasted_iota(jnp.int32, (places, rows), 0) % CAP
    sel = jnp.where(slot == place_in.astype(F32), hits, 0.0)
    sel_ref[...] = sel
    picks = (sel.astype(BF), (sel * wts).astype(BF))

    pieces = (pl.ds(0, lw), pl.ds(lw, lw))

    def to_shard(j, i, q, gp):
        v = line(i)
        return rc(send1.at[j, v, :, pieces[q]], shard.at[mine_w, g, :, pieces[q]],
                  s1s, s1r.at[q, mine_w, g], dp=gp, ep=place(v))

    def shard_in(q, v, src):
        r = shard.at[v, src, :, pieces[q]]
        return rc(r, r, s1r.at[q, v, src], s1r.at[q, v, src], ep=other)

    first = True
    for q, j, gp, buf, c in loads:
        c.wait()
        r = jnp.dot(picks[q], buf[j], preferred_element_type=F32).reshape(experts, CAP, lw).astype(BF)
        send1[j, :, :, q * lw:(q + 1) * lw] = r
        if first:
            pl.semaphore_wait(
                barrier, peers + jnp.where(pos > 0, 1, 0) + jnp.where(pos < per - 1, 1, 0))
            first = False
        for i in range(experts):
            if i or j:
                to_shard(j, i, q, gp).start()
        if j == 0:
            if experts == 1:
                shard[0, g, :, q * lw:(q + 1) * lw] = r[0]
            else:
                shard[mine_w, g, :, q * lw:(q + 1) * lw] = send1[0, mine_w, :, q * lw:(q + 1) * lw]
    for c in wloads:
        c.start()

    def at_order(k):
        m = jnp.where(pos < per - 1 - pos, pos, per - 1 - pos)
        side = jnp.where(pos < per // 2, 1, -1)
        near = pos + side * ((k + 1) // 2 if k % 2 else -(k // 2))
        far = jnp.where(pos < per - 1 - pos, k, per - 1 - k)
        return jnp.where(k <= 2 * m, near, far)

    def rows_at(h, l, c):
        return pl.ds(pl.multiple_of(((h * 2 + l) * n_dp + 2 * c) * CAP, PAIR), PAIR)

    def piece(q, h, l, c):
        return (ys if q else xs).at[rows_at(h, l, c), :]

    def pair_at(ci):
        return lax.rem(g // 2 + ci, n_pair)

    def link(h, q, c, up):
        k = q * n_pair + c
        r = piece(q, h, lo, c)
        to = e + 2 - 4 * up
        return rc(r, r, sds if up else sus, slr.at[h, k], ep=to)

    def link_in(h, q, c):
        k = q * n_pair + c
        r = piece(q, h, lo, c)
        return rc(r, r, slr.at[h, k], slr.at[h, k], ep=other)

    def fwd(h, q, c):
        k = q * n_pair + c
        r = piece(q, h, lo, c)
        return rc(r, r, sfs, sfr.at[h, k], ep=other)

    def cross(h, q, c, up):
        k = q * n_pair + c
        r = piece(q, h, 1 - lo, c)
        return rc(r, r, sds if up else sus, sfr.at[h, k], ep=e + 2 - 4 * up)

    def fwd_in(h, q, c):
        k = q * n_pair + c
        r = piece(q, h, 1 - lo, c)
        return rc(r, r, sfr.at[h, k], sfr.at[h, k], ep=other)

    def onward(h, q, c, up):
        @pl.when((pos > 0) if up else (pos < per - 1))
        def _():
            link(h, q, c, up).start()

    inner = (pos > 0) & (pos < per - 1)

    for ci in range(n_pair):
        c = pair_at(ci)
        for q in range(2):
            for i in range(experts):
                v = line(i)
                h = v * per + pos
                for b in range(2):
                    src = flip(b) if ci == 0 else 2 * c + b
                    if not (ci == 0 and b == 0 and i == 0):
                        shard_in(q, v, src).wait_recv()
                both = shard[v, pl.ds(2 * c, 2), :, q * lw:(q + 1) * lw]
                (ys if q else xs)[rows_at(h, lo, c), :] = both.astype(F32).reshape(PAIR, lw).astype(BF)
                onward(h, q, c, 0)
                onward(h, q, c, 1)
                fwd(h, q, c).start()
    pltpu.make_async_copy(w3, w3, w_sem).wait()

    def ar(b, h, part):
        bit = 1 << b
        peer = g + (1 - 2 * ((g // bit) % 2)) * bit
        src, dst = ((asx, arx), (asy, ary))[part]
        return rc(src.at[b, h], dst.at[b, h], (asxs, asys)[part], arr.at[b, h, part], dp=peer)

    def at_chunk(h):
        return pl.ds(pl.multiple_of(h * chunk, PAIR), chunk)

    def pair_rows(c):
        return pl.ds(pl.multiple_of(c * PAIR, PAIR), PAIR)

    def r1(h, c):
        return rc(rp.at[h, 1 - lo, pair_rows(c)], r1recv.at[h, pair_rows(c)], r1s, r1r.at[h, c], ep=other)

    def over(stage):
        if experts == 1:
            stage(0)
        else:
            lax.fori_loop(0, experts, lambda v, carry: (stage(v), carry)[1], 0)

    def gather_step(s, v):
        for q in range(2):
            for ci in range(n_pair):
                c = pair_at(ci)
                if s == 1:
                    @pl.when(jnp.logical_not(inner))
                    def _():
                        h = v * per + pos
                        fwd_in(h, q, c).wait_recv()
                        for up in range(2):
                            @pl.when((pos > 0) if up else (pos == 0))
                            def _():
                                cross(h, q, c, up).start()

                for up in range(2):
                    p = pos + s if up else pos - s

                    @pl.when((p <= per - 1) if up else (p >= 0))
                    def _():
                        h = v * per + p
                        link_in(h, q, c).wait_recv()
                        onward(h, q, c, up)
                        if s == 1:
                            @pl.when(jnp.logical_not(inner & ((p == 0) | (p == per - 1))))
                            def _():
                                fwd(h, q, c).start()
                        elif s == 2 or q == 0:
                            fwd(h, q, c).start()

    def cross_far(v):
        for ci in range(n_pair):
            c = pair_at(ci)

            @pl.when(inner)
            def _():
                h = v * per + at_order(per - 1)
                fwd_in(h, 1, c).wait_recv()
                for up in range(2):
                    @pl.when((pos < per // 2) if up else (pos >= per // 2))
                    def _():
                        cross(h, 1, c, up).start()

    def project(k, v):
        h = v * per + at_order(k)

        def arrived(q):
            def wait():
                for ci in range(n_pair):
                    fwd_in(h, q, pair_at(ci)).wait_recv()

            if k == 0:
                pl.when(inner)(wait)
            elif k == per - 1 and q:
                pl.when(jnp.logical_not(inner))(wait)
            else:
                wait()

        arrived(0)
        p1 = jnp.dot(xs[at_chunk(h), :], wab[...], preferred_element_type=F32)
        psx[h] = p1
        asx[0, h] = p1.astype(BF)
        ar(0, h, 0).start()
        arrived(1)
        p2 = jnp.dot(ys[at_chunk(h), :], wc[...], preferred_element_type=F32)
        psy[h] = p2
        asy[0, h] = p2.astype(BF)
        ar(0, h, 1).start()

    def reduce_step(k, b, v):
        h = v * per + at_order(k)
        for part, (ps, send, recv) in enumerate(((psx, asx, arx), (psy, asy, ary))):
            ar(b, h, part).wait_recv()
            s = ps[h] + recv[b, h].astype(F32)
            ps[h] = s
            send[b + 1, h] = s.astype(BF)
            ar(b + 1, h, part).start()

    def finish(k, v):
        h = v * per + at_order(k)
        ar(nb - 1, h, 0).wait_recv()
        s = psx[h] + arx[nb - 1, h].astype(F32)
        gate_pre, up_pre = s[:, :hid], s[:, hid:]
        sig = 1.0 / (1.0 + jnp.exp(-gate_pre))
        sw = gate_pre * sig
        hidden = (sw * up_pre).astype(BF)
        hiddens[at_chunk(h), :] = hidden
        slope = up_pre * sig * (1.0 + gate_pre * (1.0 - sig))
        ar(nb - 1, h, 1).wait_recv()
        proj = psy[h] + ary[nb - 1, h].astype(F32)
        route = jnp.sum(hidden.astype(F32) * proj, axis=1, keepdims=True)
        d1 = (proj * slope).astype(BF)
        d2 = (proj * sw).astype(BF)
        deltas[at_chunk(h), 0:hid] = d1
        deltas[at_chunk(h), hid:] = d2
        part = lax.dot_general(
            jnp.concatenate([d1, d2], axis=1), wab[...], (((1,), (1,)), ((), ())),
            preferred_element_type=F32)
        rp[h] = part.reshape(2, half, lw).astype(BF)
        rsend[h] = jnp.broadcast_to(route, (chunk, LANES)).reshape(2, n_dp, CAP, LANES).astype(BF)
        for l in range(2):
            @pl.when(h * 2 + l != e)
            def _():
                rc(rsend.at[h, l, g], rret.at[e], rts, rtr, ep=h * 2 + l).start()

            @pl.when(h * 2 + l == e)
            def _():
                rret[e] = rsend[h, l, g]

    def send_back(k, v):
        h = v * per + at_order(k)
        for ci in reversed(range(n_pair)):
            c = pair_at(ci)
            r1(h, c).wait_recv()
            both = rp[h, lo, pair_rows(c)].astype(F32) + r1recv[h, pair_rows(c)].astype(F32)
            r2send[h, pl.ds(2 * c, 2)] = both.reshape(2, CAP, lw).astype(BF)
            for b in range(2):
                gp = 2 * c + b

                def pass_on():
                    rc(r2send.at[h, gp], ret.at[hi * n_dp + g], r2s, r2r, dp=gp, ep=h * 2 + lo).start()

                def keep():
                    ret[hi * n_dp + g] = r2send[h, gp]

                if ci or (k and experts == 1):
                    pass_on()
                else:
                    mine = (h == hi) & (gp == g)
                    pl.when(jnp.logical_not(mine))(pass_on)
                    pl.when(mine)(keep)

    def G(s):
        over(functools.partial(gather_step, s))

    def P(k):
        over(functools.partial(project, k))

    def A(k):
        for b in range(nb - 1):
            over(functools.partial(reduce_step, k, b))

    def F(k):
        over(functools.partial(finish, k))

    def S(k):
        def start(v):
            for ci in reversed(range(n_pair)):
                r1(v * per + at_order(k), pair_at(ci)).start()

        over(start)

    def R(k):
        over(functools.partial(send_back, k))

    G(1)
    P(0)
    A(0)
    G(2)
    P(1)
    A(1)
    F(0)
    pl.when(inner)(functools.partial(S, 0))
    G(3)
    P(2)
    over(cross_far)
    A(2)
    F(1)
    S(1)
    P(3)
    A(3)
    F(2)
    S(2)
    R(1)
    F(3)
    S(3)
    pl.when(jnp.logical_not(inner))(functools.partial(S, 0))
    R(2)
    R(3)
    R(0)

    tile = 256 if lw % 256 == 0 else 128

    def wgrad(i, carry):
        ds = pl.ds(pl.multiple_of(i * tile, LANES), tile)
        dn = (((0,), (0,)), ((), ()))
        both = lax.dot_general(xs[:, ds], deltas[...], dn, preferred_element_type=F32).astype(BF)
        ga[ds, :] = both[:, :hid]
        gb[ds, :] = both[:, hid:]
        gc[ds, :] = lax.dot_general(ys[:, ds], hiddens[...], dn, preferred_element_type=F32).astype(BF)
        return carry

    lax.fori_loop(0, lw // tile, wgrad, 0)

    def settle(ref, sem):
        pltpu.make_async_copy(ref, ref, sem).wait()

    back, routes = ret.at[pl.ds(0, n_hi * n_dp - 1)], rret.at[pl.ds(0, n_ep - 1)]
    settle(back, r2r)
    settle(routes, rtr)
    settle(back, r2s)
    settle(routes, rts)
    settle(r1recv, r1s)
    settle(asx, asxs)
    settle(asy, asys)
    settle(xs.at[pl.ds(0, PAIR * (n_dp * experts - 1)), :], s1s)
    K = 2 * n_pair
    for at in range(per):
        ends = at in (0, per - 1)
        crossing = {0: K, per - 2: n_pair}
        down = per - 1 - at
        sent = (
            (sus, (at + 1) * K + crossing.get(at, 0) if down else 0),
            (sds, (down + 1) * K + crossing.get(down, 0) if at else 0),
            (sfs, (per - 1) * K + (n_pair if ends else 0)),
        )

        @pl.when(pos == at)
        def _(sent=sent):
            for sem, count in sent:
                if count:
                    settle(xs.at[pl.ds(0, PAIR * count * experts), :], sem)


def finish_kernel(
    ret, rret, sel_ref, ga, gb, gc, ids_ref, rw_ref, ig_hbm, rg_ref, ga_out, gb_out, gc_out,
    obuf, sem_out, osem,
):
    per = SLICES // 2
    experts = rret.shape[0] // SLICES
    n_dp = ret.shape[0] // (experts * per)
    lw = ret.shape[2]
    rows = sel_ref.shape[1]
    stride = ROUTED // experts
    outs = [
        pltpu.make_async_copy(src, dst, sem_out.at[i])
        for i, (src, dst) in enumerate(((ga, ga_out), (gb, gb_out), (gc, gc_out)))
    ]
    for c in outs:
        c.start()
    sel = sel_ref[...]
    picks = sel.astype(BF)

    def total(ref, base, step, count):
        parts = []
        for w in range(experts):
            acc = ref[w * count * step + base].astype(F32)
            for i in range(1, count):
                acc = acc + ref[(w * count + i) * step + base].astype(F32)
            parts.append(acc)
        return jnp.concatenate(parts, axis=0) if experts > 1 else parts[0]

    ocopies = []
    for j in range(n_dp):
        obuf[:, j * lw:(j + 1) * lw] = lax.dot_general(
            picks, total(ret, j, n_dp, per).astype(BF), (((0,), (0,)), ((), ())),
            preferred_element_type=F32).astype(BF)
        ds = pl.ds(j * lw, lw)
        c = pltpu.make_async_copy(obuf.at[:, ds], ig_hbm.at[:, ds], osem.at[j])
        c.start()
        ocopies.append(c)
    terms = sel * total(rret, 0, 1, SLICES)
    ids = ids_ref[...]
    rg = jnp.zeros((TOPK, rows), F32)
    for w in range(experts):
        v = jnp.sum(terms[w * CAP:(w + 1) * CAP], axis=0, keepdims=True)
        rg = rg + jnp.where(ids == w * stride, v, 0.0)
    rg_ref[...] = rg / rw_ref[...].astype(F32)
    for c in outs + ocopies:
        c.wait()


def body(tokens, out_grad, expert_ids, route_weights, gate_matrix, up_matrix, down_matrix):
    n_dp, n_ep = lax.axis_size("dp"), lax.axis_size("ep")
    experts = n_ep // SLICES
    n_hi = n_ep // 2
    n_pair = n_dp // 2
    rows, width = tokens.shape
    lw, hid = gate_matrix.shape
    nb = n_dp.bit_length() - 1
    chunk = 2 * n_dp * CAP
    half = n_dp * CAP
    total = n_hi * chunk
    K = 2 * n_pair
    V = pltpu.VMEM
    D = lambda *s: pltpu.SemaphoreType.DMA(s)
    anyspec = pl.BlockSpec(memory_space=pl.ANY)
    vspec = pl.BlockSpec(memory_space=pltpu.VMEM)
    ids, rw = expert_ids.T, route_weights.T
    grad = jax.ShapeDtypeStruct((lw, hid), BF)
    kept = pl.pallas_call(
        functools.partial(kernel, n_dp, n_ep),
        out_shape=(
            V((n_hi * n_dp, CAP, lw), BF), V((n_ep, CAP, LANES), BF), V((experts * CAP, rows), F32),
            V((lw, hid), BF), V((lw, hid), BF), V((lw, hid), BF),
        ),
        in_specs=[anyspec] * 7,
        out_specs=(vspec,) * 6,
        scratch_shapes=[
            V((TOPK, rows), jnp.int32), V((TOPK, rows), BF),
            V((n_dp, rows, lw), BF), V((n_dp, rows, lw), BF), V((lw, 3 * hid), BF),
            V((n_dp, experts, CAP, 2 * lw), BF), V((experts, n_dp, CAP, 2 * lw), BF),
            V((total, lw), BF), V((total, lw), BF),
            V((n_hi, chunk, 2 * hid), F32), V((n_hi, chunk, hid), F32),
            V((nb, n_hi, chunk, 2 * hid), BF), V((nb, n_hi, chunk, 2 * hid), BF),
            V((nb, n_hi, chunk, hid), BF), V((nb, n_hi, chunk, hid), BF),
            V((total, 2 * hid), BF), V((total, hid), BF),
            V((n_hi, 2, half, lw), BF), V((n_hi, half, lw), BF), V((n_hi, n_dp, CAP, lw), BF),
            V((n_hi, 2, n_dp, CAP, LANES), BF),
            D(2, n_dp), D(2), D(12), D(2, experts, n_dp), D(n_hi, K), D(n_hi, K), D(nb, n_hi, 2), D(n_hi, n_pair),
        ],
        compiler_params=pltpu.CompilerParams(
            collective_id=0, has_side_effects=True, vmem_limit_bytes=VMEM_BYTES),
    )(tokens, out_grad, ids, rw, gate_matrix, up_matrix, down_matrix)
    kept = [pltpu.with_memory_space_constraint(a, pltpu.VMEM) for a in kept]
    ig, rg, ga, gb, gc = pl.pallas_call(
        finish_kernel,
        out_shape=(
            jax.ShapeDtypeStruct((rows, width), BF),
            jax.ShapeDtypeStruct((TOPK, rows), F32),
            grad, grad, grad,
        ),
        in_specs=[vspec] * 8,
        out_specs=(anyspec, vspec, anyspec, anyspec, anyspec),
        scratch_shapes=[V((rows, width), BF), D(3), D(n_dp)],
        compiler_params=pltpu.CompilerParams(vmem_limit_bytes=16 * 1024 * 1024),
    )(*kept, ids, rw)
    return ig, rg.T, ga, gb, gc


def solution(mesh):
    return jax.shard_map(
        body,
        mesh=mesh,
        in_specs=(
            P(("dp", "ep"), None),
            P(("dp", "ep"), None),
            P(("dp", "ep"), None),
            P(("dp", "ep"), None),
            P("dp", "ep"),
            P("dp", "ep"),
            P("dp", "ep"),
        ),
        out_specs=(
            P(("dp", "ep"), None),
            P(("dp", "ep"), None),
            P("dp", "ep"),
            P("dp", "ep"),
            P("dp", "ep"),
        ),
        check_vma=False,
    )
```

```python
import functools
import jax
import jax.numpy as jnp
from jax import lax
from jax.experimental import pallas as pl
from jax.experimental.pallas import tpu as pltpu
from jax.sharding import PartitionSpec as P

ROUTED = 256
TOPK = 8
SLICES = 8
CAP = 8
LANES = 128
PAIR = 2 * CAP
VMEM_BYTES = 56 * 1024 * 1024
BF = jnp.bfloat16
F32 = jnp.float32
MESH = pl.DeviceIdType.MESH


def kernel(
    n_dp, n_ep,
    tok_hbm, grad_hbm, ids_hbm, rw_hbm, a_hbm, b_hbm, c_hbm,
    ret, rret, sel_ref, ga, gb, gc,
    ids_buf, rw_buf, tokbuf, gradbuf, w3, send1, shard, xs, ys,
    psx, psy, asx, arx, asy, ary, deltas, hiddens, rp, r1recv, r2send, midrecv, rsend,
    in_sem, id_sem, out_sem, s1r, slr, sfr, arr, arl, r1r, mdr,
):
    experts = n_ep // SLICES
    stride = ROUTED // experts
    places = experts * CAP
    n_hi = n_ep // 2
    per = SLICES // 2
    n_pair = n_dp // 2
    rows, width = tok_hbm.shape
    lw, hid = a_hbm.shape
    nb = n_dp.bit_length() - 1
    chunk = 2 * n_dp * CAP
    half = n_dp * CAP
    wab, wc = w3.at[:, pl.ds(0, 2 * hid)], w3.at[:, pl.ds(2 * hid, hid)]
    w_sem, s1s, sus, sds, sfs, asxs, asys, r1s, r2s, r2r, rts, rtr, mds = (out_sem.at[i] for i in range(13))
    g = lax.axis_index("dp")
    e = lax.axis_index("ep")
    hi, lo = e // 2, e % 2
    other = hi * 2 + (1 - lo)
    mine_w = hi // per
    pos = hi % per

    def rc(src, dst, ss, rs, **where):
        return pltpu.make_async_remote_copy(
            src_ref=src, dst_ref=dst, send_sem=ss, recv_sem=rs,
            device_id=where, device_id_type=MESH)

    def flip(j):
        gp = g
        for b in range(nb):
            if j >> b & 1:
                gp = gp + (1 - 2 * ((g // (1 << b)) % 2)) * (1 << b)
        return gp

    def line(i):
        return lax.rem(mine_w + i, experts)

    def place(v):
        return (v * per + pos) * 2 + lo

    id_copies = [
        pltpu.make_async_copy(ids_hbm, ids_buf, id_sem.at[0]),
        pltpu.make_async_copy(rw_hbm, rw_buf, id_sem.at[1]),
    ]
    for c in id_copies:
        c.start()
    order = list(range(1, n_dp)) + [0]
    loads = []
    for q, (src, buf) in enumerate(((tok_hbm, tokbuf), (grad_hbm, gradbuf))):
        for j in order:
            gp = flip(j)
            ds = pl.ds(pl.multiple_of(gp * lw, LANES), lw)
            c = pltpu.make_async_copy(src.at[:, ds], buf.at[j], in_sem.at[q, j])
            if q == 0:
                c.start()
            loads.append((q, j, gp, buf, c))
    wloads = [
        pltpu.make_async_copy(w, w3.at[:, pl.ds(i * hid, hid)], w_sem)
        for i, w in enumerate((a_hbm, b_hbm, c_hbm))
    ]

    barrier = pltpu.get_barrier_semaphore()
    peers = 0
    for i in range(experts):
        for j in range(n_dp):
            if i or j:
                pl.semaphore_signal(
                    barrier, inc=1, device_id={"dp": flip(j), "ep": place(line(i))}, device_id_type=MESH)
                peers += 1
    pl.semaphore_signal(barrier, inc=1, device_id={"ep": other}, device_id_type=MESH)
    peers += 1

    @pl.when(pos > 0)
    def _():
        pl.semaphore_signal(barrier, inc=1, device_id={"ep": e - 2}, device_id_type=MESH)

    @pl.when(pos < per - 1)
    def _():
        pl.semaphore_signal(barrier, inc=1, device_id={"ep": e + 2}, device_id_type=MESH)

    for c in id_copies:
        c.wait()
    for q, j, gp, buf, c in loads:
        if q:
            c.start()
    ids, rw = ids_buf[...], rw_buf[...].astype(F32)
    spread = lambda a: jnp.broadcast_to(jnp.sum(a, axis=0, keepdims=True), (CAP, rows))
    hits, wts = [], []
    for w in range(experts):
        m = ids == w * stride
        hits.append(spread(jnp.where(m, 1.0, 0.0)))
        wts.append(spread(jnp.where(m, rw, 0.0)))
    hits = jnp.concatenate(hits, axis=0) if experts > 1 else hits[0]
    wts = jnp.concatenate(wts, axis=0) if experts > 1 else wts[0]
    tr = lax.broadcasted_iota(jnp.int32, (rows, rows), 0)
    tc = lax.broadcasted_iota(jnp.int32, (rows, rows), 1)
    before = jnp.where(tr < tc, 1.0, 0.0).astype(BF)
    slot = jnp.dot(hits.astype(BF), before, preferred_element_type=F32)
    place_in = lax.broadcasted_iota(jnp.int32, (places, rows), 0) % CAP
    sel = jnp.where(slot == place_in.astype(F32), hits, 0.0)
    sel_ref[...] = sel
    picks = (sel.astype(BF), (sel * wts).astype(BF))

    pieces = (pl.ds(0, lw), pl.ds(lw, lw))

    def to_shard(j, i, q, gp):
        v = line(i)
        return rc(send1.at[j, v, :, pieces[q]], shard.at[mine_w, g, :, pieces[q]],
                  s1s, s1r.at[q, mine_w, g], dp=gp, ep=place(v))

    def shard_in(q, v, src):
        r = shard.at[v, src, :, pieces[q]]
        return rc(r, r, s1r.at[q, v, src], s1r.at[q, v, src], ep=other)

    first = True
    for q, j, gp, buf, c in loads:
        c.wait()
        r = jnp.dot(picks[q], buf[j], preferred_element_type=F32).reshape(experts, CAP, lw).astype(BF)
        send1[j, :, :, q * lw:(q + 1) * lw] = r
        if first:
            pl.semaphore_wait(
                barrier, peers + jnp.where(pos > 0, 1, 0) + jnp.where(pos < per - 1, 1, 0))
            first = False
        for i in range(experts):
            if i or j:
                to_shard(j, i, q, gp).start()
        if j == 0:
            if experts == 1:
                shard[0, g, :, q * lw:(q + 1) * lw] = r[0]
            else:
                shard[mine_w, g, :, q * lw:(q + 1) * lw] = send1[0, mine_w, :, q * lw:(q + 1) * lw]
    for c in wloads:
        c.start()

    def at_order(k):
        m = jnp.where(pos < per - 1 - pos, pos, per - 1 - pos)
        side = jnp.where(pos < per // 2, 1, -1)
        near = pos + side * ((k + 1) // 2 if k % 2 else -(k // 2))
        far = jnp.where(pos < per - 1 - pos, k, per - 1 - k)
        return jnp.where(k <= 2 * m, near, far)

    def rows_at(h, l, c):
        return pl.ds(pl.multiple_of(((h * 2 + l) * n_dp + 2 * c) * CAP, PAIR), PAIR)

    def piece(q, h, l, c):
        return (ys if q else xs).at[rows_at(h, l, c), :]

    def pair_at(ci):
        return lax.rem(g // 2 + ci, n_pair)

    def link(h, q, c, up):
        k = q * n_pair + c
        r = piece(q, h, lo, c)
        to = e + 2 - 4 * up
        return rc(r, r, sds if up else sus, slr.at[h, k], ep=to)

    def link_in(h, q, c):
        k = q * n_pair + c
        r = piece(q, h, lo, c)
        return rc(r, r, slr.at[h, k], slr.at[h, k], ep=other)

    def fwd(h, q, c):
        k = q * n_pair + c
        r = piece(q, h, lo, c)
        return rc(r, r, sfs, sfr.at[h, k], ep=other)

    def cross(h, q, c, up):
        k = q * n_pair + c
        r = piece(q, h, 1 - lo, c)
        return rc(r, r, sds if up else sus, sfr.at[h, k], ep=e + 2 - 4 * up)

    def fwd_in(h, q, c):
        k = q * n_pair + c
        r = piece(q, h, 1 - lo, c)
        return rc(r, r, sfr.at[h, k], sfr.at[h, k], ep=other)

    def onward(h, q, c, up):
        @pl.when((pos > 0) if up else (pos < per - 1))
        def _():
            link(h, q, c, up).start()

    inner = (pos > 0) & (pos < per - 1)

    for ci in range(n_pair):
        c = pair_at(ci)
        for q in range(2):
            for i in range(experts):
                v = line(i)
                h = v * per + pos
                for b in range(2):
                    src = flip(b) if ci == 0 else 2 * c + b
                    if not (ci == 0 and b == 0 and i == 0):
                        shard_in(q, v, src).wait_recv()
                both = shard[v, pl.ds(2 * c, 2), :, q * lw:(q + 1) * lw]
                (ys if q else xs)[rows_at(h, lo, c), :] = both.astype(F32).reshape(PAIR, lw).astype(BF)
                onward(h, q, c, 0)
                onward(h, q, c, 1)
                fwd(h, q, c).start()
    pltpu.make_async_copy(w3, w3, w_sem).wait()

    def half_at(late):
        return pl.ds(pl.multiple_of((1 - lo if late else lo) * half, PAIR), half)

    def ar(b, k, v, part, late):
        h = v * per + at_order(k)
        bit = 1 << b
        peer = g + (1 - 2 * ((g // bit) % 2)) * bit
        src, dst = (r.at[b, h] if late is None else r.at[b, h, half_at(late)] for r in ((asx, arx), (asy, ary))[part])
        sem = arl.at[b, k - 1, v, part] if late else arr.at[b, h, part]
        return rc(src, dst, (asxs, asys)[part], sem, dp=peer)

    def at_chunk(h):
        return pl.ds(pl.multiple_of(h * chunk, PAIR), chunk)

    def pair_rows(c):
        return pl.ds(pl.multiple_of(c * PAIR, PAIR), PAIR)

    left = (lw // LANES + 1) // 2 * LANES
    cols = (pl.ds(0, left), pl.ds(left, lw - left))

    def r1(h, c, m):
        return rc(rp.at[h, 1 - lo, pair_rows(c), cols[m]], r1recv.at[h, pair_rows(c), cols[m]],
                  r1s, r1r.at[h, c, m], ep=other)

    def over(stage):
        if experts == 1:
            stage(0)
        else:
            lax.fori_loop(0, experts, lambda v, carry: (stage(v), carry)[1], 0)

    def gather_step(s, qs, v):
        for q in qs:
            for ci in range(n_pair):
                c = pair_at(ci)
                if s == 1:
                    @pl.when(jnp.logical_not(inner))
                    def _():
                        h = v * per + pos
                        fwd_in(h, q, c).wait_recv()
                        for up in range(2):
                            @pl.when((pos > 0) if up else (pos == 0))
                            def _():
                                cross(h, q, c, up).start()

                for up in range(2):
                    p = pos + s if up else pos - s

                    @pl.when((p <= per - 1) if up else (p >= 0))
                    def _():
                        h = v * per + p
                        link_in(h, q, c).wait_recv()
                        onward(h, q, c, up)
                        if s == 1:
                            @pl.when(jnp.logical_not(inner & ((p == 0) | (p == per - 1))))
                            def _():
                                fwd(h, q, c).start()
                        elif s == 2 and q == 0:
                            @pl.when(jnp.logical_not(inner))
                            def _():
                                fwd(h, q, c).start()
                        elif s == 2 or q == 0:
                            fwd(h, q, c).start()

    def cross_on(k, q, away, v):
        h = v * per + at_order(k)
        for ci in range(n_pair):
            c = pair_at(ci)
            fwd_in(h, q, c).wait_recv()
            for up in range(2):
                @pl.when((pos < per // 2) == (up == away))
                def _():
                    cross(h, q, c, up).start()

    def rows_in(h, late):
        if late is None:
            return at_chunk(h)
        return pl.ds(pl.multiple_of(h * chunk + (1 - lo if late else lo) * half, PAIR), half)

    def project(k, late, v):
        h = v * per + at_order(k)

        def arrived(q):
            def wait():
                for ci in range(n_pair):
                    fwd_in(h, q, pair_at(ci)).wait_recv()

            if late is False:
                return
            if k == 0:
                pl.when(inner)(wait)
            elif (k, q) in ((per - 2, 0), (per - 1, 1)):
                pl.when(jnp.logical_not(inner))(wait)
            else:
                wait()

        for part, (rows_of, w, ps, send) in enumerate(((xs, wab, psx, asx), (ys, wc, psy, asy))):
            arrived(part)
            p = jnp.dot(rows_of[rows_in(h, late), :], w[...], preferred_element_type=F32)
            if late is None:
                ps[h] = p
                send[0, h] = p.astype(BF)
            else:
                ps[h, half_at(late)] = p
                send[0, h, half_at(late)] = p.astype(BF)
            ar(0, k, v, part, late).start()

    def reduce_step(k, b, late, v):
        h = v * per + at_order(k)
        for part, (ps, send, recv) in enumerate(((psx, asx, arx), (psy, asy, ary))):
            ar(b, k, v, part, late).wait_recv()
            if late is None:
                s = ps[h] + recv[b, h].astype(F32)
                ps[h] = s
                send[b + 1, h] = s.astype(BF)
            else:
                r = half_at(late)
                s = ps[h, r] + recv[b, h, r].astype(F32)
                ps[h, r] = s
                send[b + 1, h, r] = s.astype(BF)
            ar(b + 1, k, v, part, late).start()

    def start_back(k, m, v):
        for ci in reversed(range(n_pair)):
            r1(v * per + at_order(k), pair_at(ci), m).start()

    def to_middle(h, v, m):
        return rc(rp.at[h, :, :, cols[m]], midrecv.at[v, :, :, cols[m]], mds, mdr.at[v, m],
                  ep=e + jnp.where(pos < per // 2, 2, -2))

    def merge(v):
        h = v * per + pos
        for m, at in enumerate(cols):
            to_middle(h, v, m).wait_recv()
            rp[h, :, :, at] = (rp[h, :, :, at].astype(F32) + midrecv[v, :, :, at].astype(F32)).astype(BF)
            start_back(0, m, v)

    def finish(k, lates, middle, v):
        h = v * per + at_order(k)
        for late in lates:
            ar(nb - 1, k, v, 0, late).wait_recv()
        s = psx[h] + arx[nb - 1, h].astype(F32)
        gate_pre, up_pre = s[:, :hid], s[:, hid:]
        sig = 1.0 / (1.0 + jnp.exp(-gate_pre))
        sw = gate_pre * sig
        hidden = (sw * up_pre).astype(BF)
        hiddens[at_chunk(h), :] = hidden
        slope = up_pre * sig * (1.0 + gate_pre * (1.0 - sig))
        for late in lates:
            ar(nb - 1, k, v, 1, late).wait_recv()
        proj = psy[h] + ary[nb - 1, h].astype(F32)
        route = jnp.sum(hidden.astype(F32) * proj, axis=1, keepdims=True)
        d1 = (proj * slope).astype(BF)
        d2 = (proj * sw).astype(BF)
        deltas[at_chunk(h), 0:hid] = d1
        deltas[at_chunk(h), hid:] = d2
        both = jnp.concatenate([d1, d2], axis=1)
        for m, at in enumerate(cols):
            part = lax.dot_general(
                both, wab[at, :], (((1,), (1,)), ((), ())), preferred_element_type=F32)
            rp[h, :, :, at] = part.reshape(2, half, part.shape[1]).astype(BF)
            if middle:
                to_middle(h, v, m).start()
            elif k:
                start_back(k, m, v)
        rsend[h] = jnp.broadcast_to(route, (chunk, LANES)).reshape(2, n_dp, CAP, LANES).astype(BF)
        for l in range(2):
            @pl.when(h * 2 + l != e)
            def _():
                rc(rsend.at[h, l, g], rret.at[e], rts, rtr, ep=h * 2 + l).start()

            @pl.when(h * 2 + l == e)
            def _():
                rret[e] = rsend[h, l, g]

    def send_back(k, v):
        h = v * per + at_order(k)
        for m, at in enumerate(cols):
            for ci in reversed(range(n_pair)):
                c = pair_at(ci)
                r1(h, c, m).wait_recv()
                both = rp[h, lo, pair_rows(c), at].astype(F32) + r1recv[h, pair_rows(c), at].astype(F32)
                r2send[h, pl.ds(2 * c, 2), :, at] = both.reshape(2, CAP, both.shape[1]).astype(BF)
                for b in range(2):
                    gp = 2 * c + b

                    def pass_on():
                        rc(r2send.at[h, gp, :, at], ret.at[hi * n_dp + g, :, at], r2s, r2r,
                           dp=gp, ep=h * 2 + lo).start()

                    def keep():
                        ret[hi * n_dp + g, :, at] = r2send[h, gp, :, at]

                    if ci or (k and experts == 1):
                        pass_on()
                    else:
                        mine = (h == hi) & (gp == g)
                        pl.when(jnp.logical_not(mine))(pass_on)
                        pl.when(mine)(keep)

    def G(s, *qs):
        over(functools.partial(gather_step, s, qs))

    def X(k, q, away):
        over(functools.partial(cross_on, k, q, away))

    def P(k, late=None):
        over(functools.partial(project, k, late))

    def A(k, late=None):
        for b in range(nb - 1):
            over(functools.partial(reduce_step, k, b, late))

    def F(k, *lates, middle=False):
        over(functools.partial(finish, k, lates or (None,), middle))

    def S(k, *parts):
        for m in parts:
            over(functools.partial(start_back, k, m))

    def R(k):
        over(functools.partial(send_back, k))

    tile = 256 if lw % 256 == 0 else 128
    tiles = lw // tile

    def wgrad(i, carry):
        ds = pl.ds(pl.multiple_of(i * tile, LANES), tile)
        dn = (((0,), (0,)), ((), ()))
        both = lax.dot_general(xs[:, ds], deltas[...], dn, preferred_element_type=F32).astype(BF)
        ga[ds, :] = both[:, :hid]
        gb[ds, :] = both[:, hid:]
        gc[ds, :] = lax.dot_general(ys[:, ds], hiddens[...], dn, preferred_element_type=F32).astype(BF)
        return carry

    def W(part):
        lax.fori_loop((0, (tiles + 1) // 2)[part], ((tiles + 1) // 2, tiles)[part], wgrad, 0)

    G(1, 0, 1)
    P(0)
    A(0)

    @pl.when(inner)
    def _():
        P(1, False)
        G(2, 0)
        A(1, False)
        X(2, 0, 0)
        P(1, True)
        G(2, 1)
        F(0)
        A(1, True)
        P(3, False)
        P(2)
        A(3, False)
        X(3, 1, 1)
        P(3, True)
        A(3, True)
        F(1, False, True, middle=True)
        A(2)
        F(3, False, True)
        F(2)
        R(3)
        over(merge)
        W(0)
        R(2)
        W(1)
        R(0)

    @pl.when(jnp.logical_not(inner))
    def _():
        G(2, 0, 1)
        P(1)
        A(1)
        F(0)
        G(3, 0)
        P(2, False)
        A(2, False)
        P(2, True)
        G(3, 1)
        S(0, 0)
        P(3, False)
        A(2, True)
        F(1)
        A(3, False)
        P(3, True)
        A(3, True)
        F(2, False, True)
        R(1)
        F(3, False, True)
        W(0)
        R(2)
        S(0, 1)
        R(3)
        R(0)
        W(1)

    def settle(ref, sem):
        pltpu.make_async_copy(ref, ref, sem).wait()

    def settle_back(sem):
        for group, fewer in ((inner, experts * n_dp), (jnp.logical_not(inner), 0)):
            @pl.when(group)
            def _():
                settle(ret.at[pl.ds(0, n_hi * n_dp - 1 - fewer)], sem)

    routes = rret.at[pl.ds(0, n_ep - 1)]
    settle_back(r2r)
    settle(routes, rtr)
    settle_back(r2s)
    settle(routes, rts)

    @pl.when(inner)
    def _():
        settle(r1recv.at[pl.ds(0, n_hi - experts)], r1s)
        settle(midrecv, mds)
        for w in range(experts):
            unused = (w * per + per - 1 - pos) * n_dp
            ret[pl.ds(unused, n_dp)] = jnp.zeros((n_dp, CAP, lw), BF)

    @pl.when(jnp.logical_not(inner))
    def _():
        settle(r1recv, r1s)

    settle(asx, asxs)
    settle(asy, asys)
    settle(xs.at[pl.ds(0, PAIR * (n_dp * experts - 1)), :], s1s)
    K = 2 * n_pair
    for at in range(per):
        ends = at in (0, per - 1)
        down = per - 1 - at
        crossing = lambda behind: n_pair if behind else K
        sent = (
            (sus, (at + 1) * K + crossing(at) if down else 0),
            (sds, (down + 1) * K + crossing(down) if at else 0),
            (sfs, (per - 1 if ends else per - 2) * K + n_pair),
        )

        @pl.when(pos == at)
        def _(sent=sent):
            for sem, count in sent:
                if count:
                    settle(xs.at[pl.ds(0, PAIR * count * experts), :], sem)


def finish_kernel(
    ret, rret, sel_ref, ga, gb, gc, ids_ref, rw_ref, ig_hbm, rg_ref, ga_out, gb_out, gc_out,
    obuf, sem_out, osem,
):
    per = SLICES // 2
    experts = rret.shape[0] // SLICES
    n_dp = ret.shape[0] // (experts * per)
    lw = ret.shape[2]
    rows = sel_ref.shape[1]
    stride = ROUTED // experts
    outs = [
        pltpu.make_async_copy(src, dst, sem_out.at[i])
        for i, (src, dst) in enumerate(((ga, ga_out), (gb, gb_out), (gc, gc_out)))
    ]
    for c in outs:
        c.start()
    sel = sel_ref[...]
    picks = sel.astype(BF)

    def total(ref, base, step, count):
        parts = []
        for w in range(experts):
            acc = ref[w * count * step + base].astype(F32)
            for i in range(1, count):
                acc = acc + ref[(w * count + i) * step + base].astype(F32)
            parts.append(acc)
        return jnp.concatenate(parts, axis=0) if experts > 1 else parts[0]

    ocopies = []
    for j in range(n_dp):
        obuf[:, j * lw:(j + 1) * lw] = lax.dot_general(
            picks, total(ret, j, n_dp, per).astype(BF), (((0,), (0,)), ((), ())),
            preferred_element_type=F32).astype(BF)
        ds = pl.ds(j * lw, lw)
        c = pltpu.make_async_copy(obuf.at[:, ds], ig_hbm.at[:, ds], osem.at[j])
        c.start()
        ocopies.append(c)
    terms = sel * total(rret, 0, 1, SLICES)
    ids = ids_ref[...]
    rg = jnp.zeros((TOPK, rows), F32)
    for w in range(experts):
        v = jnp.sum(terms[w * CAP:(w + 1) * CAP], axis=0, keepdims=True)
        rg = rg + jnp.where(ids == w * stride, v, 0.0)
    rg_ref[...] = rg / rw_ref[...].astype(F32)
    for c in outs + ocopies:
        c.wait()


def body(tokens, out_grad, expert_ids, route_weights, gate_matrix, up_matrix, down_matrix):
    n_dp, n_ep = lax.axis_size("dp"), lax.axis_size("ep")
    experts = n_ep // SLICES
    n_hi = n_ep // 2
    n_pair, per = n_dp // 2, SLICES // 2
    rows, width = tokens.shape
    lw, hid = gate_matrix.shape
    nb = n_dp.bit_length() - 1
    chunk = 2 * n_dp * CAP
    half = n_dp * CAP
    total = n_hi * chunk
    K = 2 * n_pair
    V = pltpu.VMEM
    D = lambda *s: pltpu.SemaphoreType.DMA(s)
    anyspec = pl.BlockSpec(memory_space=pl.ANY)
    vspec = pl.BlockSpec(memory_space=pltpu.VMEM)
    ids, rw = expert_ids.T, route_weights.T
    grad = jax.ShapeDtypeStruct((lw, hid), BF)
    kept = pl.pallas_call(
        functools.partial(kernel, n_dp, n_ep),
        out_shape=(
            V((n_hi * n_dp, CAP, lw), BF), V((n_ep, CAP, LANES), BF), V((experts * CAP, rows), F32),
            V((lw, hid), BF), V((lw, hid), BF), V((lw, hid), BF),
        ),
        in_specs=[anyspec] * 7,
        out_specs=(vspec,) * 6,
        scratch_shapes=[
            V((TOPK, rows), jnp.int32), V((TOPK, rows), BF),
            V((n_dp, rows, lw), BF), V((n_dp, rows, lw), BF), V((lw, 3 * hid), BF),
            V((n_dp, experts, CAP, 2 * lw), BF), V((experts, n_dp, CAP, 2 * lw), BF),
            V((total, lw), BF), V((total, lw), BF),
            V((n_hi, chunk, 2 * hid), F32), V((n_hi, chunk, hid), F32),
            V((nb, n_hi, chunk, 2 * hid), BF), V((nb, n_hi, chunk, 2 * hid), BF),
            V((nb, n_hi, chunk, hid), BF), V((nb, n_hi, chunk, hid), BF),
            V((total, 2 * hid), BF), V((total, hid), BF),
            V((n_hi, 2, half, lw), BF), V((n_hi, half, lw), BF), V((n_hi, n_dp, CAP, lw), BF),
            V((experts, 2, half, lw), BF),
            V((n_hi, 2, n_dp, CAP, LANES), BF),
            D(2, n_dp), D(2), D(13), D(2, experts, n_dp), D(n_hi, K), D(n_hi, K), D(nb, n_hi, 2), D(nb, per - 1, experts, 2), D(n_hi, n_pair, 2), D(experts, 2),
        ],
        compiler_params=pltpu.CompilerParams(
            collective_id=0, has_side_effects=True, vmem_limit_bytes=VMEM_BYTES),
    )(tokens, out_grad, ids, rw, gate_matrix, up_matrix, down_matrix)
    kept = [pltpu.with_memory_space_constraint(a, pltpu.VMEM) for a in kept]
    ig, rg, ga, gb, gc = pl.pallas_call(
        finish_kernel,
        out_shape=(
            jax.ShapeDtypeStruct((rows, width), BF),
            jax.ShapeDtypeStruct((TOPK, rows), F32),
            grad, grad, grad,
        ),
        in_specs=[vspec] * 8,
        out_specs=(anyspec, vspec, anyspec, anyspec, anyspec),
        scratch_shapes=[V((rows, width), BF), D(3), D(n_dp)],
        compiler_params=pltpu.CompilerParams(vmem_limit_bytes=16 * 1024 * 1024),
    )(*kept, ids, rw)
    return ig, rg.T, ga, gb, gc


def solution(mesh):
    return jax.shard_map(
        body,
        mesh=mesh,
        in_specs=(
            P(("dp", "ep"), None),
            P(("dp", "ep"), None),
            P(("dp", "ep"), None),
            P(("dp", "ep"), None),
            P("dp", "ep"),
            P("dp", "ep"),
            P("dp", "ep"),
        ),
        out_specs=(
            P(("dp", "ep"), None),
            P(("dp", "ep"), None),
            P("dp", "ep"),
            P("dp", "ep"),
            P("dp", "ep"),
        ),
        check_vma=False,
    )
```

```python
import functools
import jax
import jax.numpy as jnp
from jax import lax
from jax.experimental import pallas as pl
from jax.experimental.pallas import tpu as pltpu
from jax.sharding import PartitionSpec as P

ROUTED = 256
TOPK = 8
SLICES = 8
CAP = 8
LANES = 128
PAIR = 2 * CAP
VMEM_BYTES = 56 * 1024 * 1024
BF = jnp.bfloat16
F32 = jnp.float32
MESH = pl.DeviceIdType.MESH


def kernel(
    n_dp, n_ep,
    tok_hbm, grad_hbm, ids_hbm, rw_hbm, a_hbm, b_hbm, c_hbm,
    ret, rret, sel_ref, ga, gb, gc,
    ids_buf, rw_buf, tokbuf, gradbuf, w3, send1, shard, xs, ys,
    psx, psy, asx, arx, asy, ary, deltas, hiddens, rp, r1recv, r2send, midrecv, rsend,
    in_sem, id_sem, out_sem, s1r, slr, sfr, arr, arl, r1r, mdr,
):
    experts = n_ep // SLICES
    stride = ROUTED // experts
    places = experts * CAP
    n_hi = n_ep // 2
    per = SLICES // 2
    n_pair = n_dp // 2
    rows, width = tok_hbm.shape
    lw, hid = a_hbm.shape
    nb = n_dp.bit_length() - 1
    chunk = 2 * n_dp * CAP
    half = n_dp * CAP
    wab, wc = w3.at[:, pl.ds(0, 2 * hid)], w3.at[:, pl.ds(2 * hid, hid)]
    w_sem, s1s, sus, sds, sfs, asxs, asys, r1s, r2s, r2r, rts, rtr, mds = (out_sem.at[i] for i in range(13))
    g = lax.axis_index("dp")
    e = lax.axis_index("ep")
    hi, lo = e // 2, e % 2
    other = hi * 2 + (1 - lo)
    mine_w = hi // per
    pos = hi % per

    def rc(src, dst, ss, rs, **where):
        return pltpu.make_async_remote_copy(
            src_ref=src, dst_ref=dst, send_sem=ss, recv_sem=rs,
            device_id=where, device_id_type=MESH)

    def flip(j):
        gp = g
        for b in range(nb):
            if j >> b & 1:
                gp = gp + (1 - 2 * ((g // (1 << b)) % 2)) * (1 << b)
        return gp

    def line(i):
        return lax.rem(mine_w + i, experts)

    def place(v):
        return (v * per + pos) * 2 + lo

    id_copies = [
        pltpu.make_async_copy(ids_hbm, ids_buf, id_sem.at[0]),
        pltpu.make_async_copy(rw_hbm, rw_buf, id_sem.at[1]),
    ]
    for c in id_copies:
        c.start()
    order = list(range(2, n_dp)) + [1, 0]
    loads = []
    for q, (src, buf) in enumerate(((tok_hbm, tokbuf), (grad_hbm, gradbuf))):
        for j in order:
            gp = flip(j)
            ds = pl.ds(pl.multiple_of(gp * lw, LANES), lw)
            c = pltpu.make_async_copy(src.at[:, ds], buf.at[j], in_sem.at[q, j])
            if q == 0:
                c.start()
            loads.append((q, j, gp, buf, c))
    wloads = [
        pltpu.make_async_copy(w, w3.at[:, pl.ds(i * hid, hid)], w_sem)
        for i, w in enumerate((a_hbm, b_hbm, c_hbm))
    ]

    barrier = pltpu.get_barrier_semaphore()
    peers = 0
    for i in range(experts):
        for j in range(n_dp):
            if i or j:
                pl.semaphore_signal(
                    barrier, inc=1, device_id={"dp": flip(j), "ep": place(line(i))}, device_id_type=MESH)
                peers += 1
    pl.semaphore_signal(barrier, inc=1, device_id={"ep": other}, device_id_type=MESH)
    peers += 1

    @pl.when(pos > 0)
    def _():
        pl.semaphore_signal(barrier, inc=1, device_id={"ep": e - 2}, device_id_type=MESH)

    @pl.when(pos < per - 1)
    def _():
        pl.semaphore_signal(barrier, inc=1, device_id={"ep": e + 2}, device_id_type=MESH)

    for c in id_copies:
        c.wait()
    for q, j, gp, buf, c in loads:
        if q:
            c.start()
    ids, rw = ids_buf[...], rw_buf[...].astype(F32)
    spread = lambda a: jnp.broadcast_to(jnp.sum(a, axis=0, keepdims=True), (CAP, rows))
    hits, wts = [], []
    for w in range(experts):
        m = ids == w * stride
        hits.append(spread(jnp.where(m, 1.0, 0.0)))
        wts.append(spread(jnp.where(m, rw, 0.0)))
    hits = jnp.concatenate(hits, axis=0) if experts > 1 else hits[0]
    wts = jnp.concatenate(wts, axis=0) if experts > 1 else wts[0]
    tr = lax.broadcasted_iota(jnp.int32, (rows, rows), 0)
    tc = lax.broadcasted_iota(jnp.int32, (rows, rows), 1)
    before = jnp.where(tr < tc, 1.0, 0.0).astype(BF)
    slot = jnp.dot(hits.astype(BF), before, preferred_element_type=F32)
    place_in = lax.broadcasted_iota(jnp.int32, (places, rows), 0) % CAP
    sel = jnp.where(slot == place_in.astype(F32), hits, 0.0)
    sel_ref[...] = sel
    picks = (sel.astype(BF), (sel * wts).astype(BF))

    pieces = (pl.ds(0, lw), pl.ds(lw, lw))

    def to_shard(j, i, q, gp):
        v = line(i)
        return rc(send1.at[j, v, :, pieces[q]], shard.at[mine_w, g, :, pieces[q]],
                  s1s, s1r.at[q, mine_w, g], dp=gp, ep=place(v))

    def shard_in(q, v, src):
        r = shard.at[v, src, :, pieces[q]]
        return rc(r, r, s1r.at[q, v, src], s1r.at[q, v, src], ep=other)

    first = True
    for q, j, gp, buf, c in loads:
        c.wait()
        r = jnp.dot(picks[q], buf[j], preferred_element_type=F32).reshape(experts, CAP, lw).astype(BF)
        send1[j, :, :, q * lw:(q + 1) * lw] = r
        if first:
            pl.semaphore_wait(
                barrier, peers + jnp.where(pos > 0, 1, 0) + jnp.where(pos < per - 1, 1, 0))
            first = False
        for i in range(experts):
            if i or j:
                to_shard(j, i, q, gp).start()
        if j == 0:
            if experts == 1:
                shard[0, g, :, q * lw:(q + 1) * lw] = r[0]
            else:
                shard[mine_w, g, :, q * lw:(q + 1) * lw] = send1[0, mine_w, :, q * lw:(q + 1) * lw]
    for c in wloads:
        c.start()

    def at_order(k):
        m = jnp.where(pos < per - 1 - pos, pos, per - 1 - pos)
        side = jnp.where(pos < per // 2, 1, -1)
        near = pos + side * ((k + 1) // 2 if k % 2 else -(k // 2))
        far = jnp.where(pos < per - 1 - pos, k, per - 1 - k)
        return jnp.where(k <= 2 * m, near, far)

    def rows_at(h, l, c):
        return pl.ds(pl.multiple_of(((h * 2 + l) * n_dp + 2 * c) * CAP, PAIR), PAIR)

    def piece(q, h, l, c):
        return (ys if q else xs).at[rows_at(h, l, c), :]

    def pair_at(ci):
        return lax.rem(g // 2 + ci, n_pair)

    def link(h, q, c, up):
        k = q * n_pair + c
        r = piece(q, h, lo, c)
        to = e + 2 - 4 * up
        return rc(r, r, sds if up else sus, slr.at[h, k], ep=to)

    def link_in(h, q, c):
        k = q * n_pair + c
        r = piece(q, h, lo, c)
        return rc(r, r, slr.at[h, k], slr.at[h, k], ep=other)

    def fwd(h, q, c):
        k = q * n_pair + c
        r = piece(q, h, lo, c)
        return rc(r, r, sfs, sfr.at[h, k], ep=other)

    def cross(h, q, c, up):
        k = q * n_pair + c
        r = piece(q, h, 1 - lo, c)
        return rc(r, r, sds if up else sus, sfr.at[h, k], ep=e + 2 - 4 * up)

    def fwd_in(h, q, c):
        k = q * n_pair + c
        r = piece(q, h, 1 - lo, c)
        return rc(r, r, sfr.at[h, k], sfr.at[h, k], ep=other)

    def onward(h, q, c, up):
        @pl.when((pos > 0) if up else (pos < per - 1))
        def _():
            link(h, q, c, up).start()

    inner = (pos > 0) & (pos < per - 1)

    for ci in range(n_pair):
        c = pair_at(ci)
        for q in range(2):
            for i in range(experts):
                v = line(i)
                h = v * per + pos
                for b in range(2):
                    src = flip(b) if ci == 0 else 2 * c + b
                    if not (ci == 0 and b == 0 and i == 0):
                        shard_in(q, v, src).wait_recv()
                both = shard[v, pl.ds(2 * c, 2), :, q * lw:(q + 1) * lw]
                (ys if q else xs)[rows_at(h, lo, c), :] = both.astype(F32).reshape(PAIR, lw).astype(BF)
                onward(h, q, c, 0)
                onward(h, q, c, 1)
                fwd(h, q, c).start()
    pltpu.make_async_copy(w3, w3, w_sem).wait()

    def half_at(late):
        return pl.ds(pl.multiple_of((1 - lo if late else lo) * half, PAIR), half)

    def ar(b, k, v, part, late):
        h = v * per + at_order(k)
        bit = 1 << b
        peer = g + (1 - 2 * ((g // bit) % 2)) * bit
        src, dst = (r.at[b, h] if late is None else r.at[b, h, half_at(late)] for r in ((asx, arx), (asy, ary))[part])
        sem = arl.at[b, k - 1, v, part] if late else arr.at[b, h, part]
        return rc(src, dst, (asxs, asys)[part], sem, dp=peer)

    def at_chunk(h):
        return pl.ds(pl.multiple_of(h * chunk, PAIR), chunk)

    def pair_rows(c):
        return pl.ds(pl.multiple_of(c * PAIR, PAIR), PAIR)

    left = (lw // LANES + 1) // 2 * LANES
    cols = (pl.ds(0, left), pl.ds(left, lw - left))

    def r1(h, c, m):
        return rc(rp.at[h, 1 - lo, pair_rows(c), cols[m]], r1recv.at[h, pair_rows(c), cols[m]],
                  r1s, r1r.at[h, c, m], ep=other)

    def over(stage):
        if experts == 1:
            stage(0)
        else:
            lax.fori_loop(0, experts, lambda v, carry: (stage(v), carry)[1], 0)

    def gather_step(s, qs, v):
        for q in qs:
            for ci in range(n_pair):
                c = pair_at(ci)
                if s == 1:
                    @pl.when(jnp.logical_not(inner))
                    def _():
                        h = v * per + pos
                        fwd_in(h, q, c).wait_recv()
                        for up in range(2):
                            @pl.when((pos > 0) if up else (pos == 0))
                            def _():
                                cross(h, q, c, up).start()

                for up in range(2):
                    p = pos + s if up else pos - s

                    @pl.when((p <= per - 1) if up else (p >= 0))
                    def _():
                        h = v * per + p
                        link_in(h, q, c).wait_recv()
                        onward(h, q, c, up)
                        if s == 1:
                            @pl.when(jnp.logical_not(inner & ((p == 0) | (p == per - 1))))
                            def _():
                                fwd(h, q, c).start()
                        elif s == 2 and q == 0:
                            @pl.when(jnp.logical_not(inner))
                            def _():
                                fwd(h, q, c).start()
                        elif s == 2 or q == 0:
                            fwd(h, q, c).start()

    def cross_on(k, q, away, v):
        h = v * per + at_order(k)
        for ci in range(n_pair):
            c = pair_at(ci)
            fwd_in(h, q, c).wait_recv()
            for up in range(2):
                @pl.when((pos < per // 2) == (up == away))
                def _():
                    cross(h, q, c, up).start()

    def rows_in(h, late):
        if late is None:
            return at_chunk(h)
        return pl.ds(pl.multiple_of(h * chunk + (1 - lo if late else lo) * half, PAIR), half)

    def project(k, late, v):
        h = v * per + at_order(k)

        def arrived(q):
            def wait():
                for ci in range(n_pair):
                    fwd_in(h, q, pair_at(ci)).wait_recv()

            if late is False:
                return
            if k == 0:
                pl.when(inner)(wait)
            elif (k, q) in ((per - 2, 0), (per - 1, 1)):
                pl.when(jnp.logical_not(inner))(wait)
            else:
                wait()

        for part, (rows_of, w, ps, send) in enumerate(((xs, wab, psx, asx), (ys, wc, psy, asy))):
            arrived(part)
            p = jnp.dot(rows_of[rows_in(h, late), :], w[...], preferred_element_type=F32)
            if late is None:
                ps[h] = p
                send[0, h] = p.astype(BF)
            else:
                ps[h, half_at(late)] = p
                send[0, h, half_at(late)] = p.astype(BF)
            ar(0, k, v, part, late).start()

    def reduce_step(k, b, late, v):
        h = v * per + at_order(k)
        for part, (ps, send, recv) in enumerate(((psx, asx, arx), (psy, asy, ary))):
            ar(b, k, v, part, late).wait_recv()
            if late is None:
                s = ps[h] + recv[b, h].astype(F32)
                ps[h] = s
                send[b + 1, h] = s.astype(BF)
            else:
                r = half_at(late)
                s = ps[h, r] + recv[b, h, r].astype(F32)
                ps[h, r] = s
                send[b + 1, h, r] = s.astype(BF)
            ar(b + 1, k, v, part, late).start()

    def start_back(k, m, v):
        for ci in reversed(range(n_pair)):
            r1(v * per + at_order(k), pair_at(ci), m).start()

    def to_middle(h, v, m):
        return rc(rp.at[h, :, :, cols[m]], midrecv.at[v, :, :, cols[m]], mds, mdr.at[v, m],
                  ep=e + jnp.where(pos < per // 2, 2, -2))

    def merge(v):
        h = v * per + pos
        for m, at in enumerate(cols):
            to_middle(h, v, m).wait_recv()
            rp[h, :, :, at] = (rp[h, :, :, at].astype(F32) + midrecv[v, :, :, at].astype(F32)).astype(BF)
            start_back(0, m, v)

    def finish(k, lates, middle, v):
        h = v * per + at_order(k)
        for late in lates:
            ar(nb - 1, k, v, 0, late).wait_recv()
        s = psx[h] + arx[nb - 1, h].astype(F32)
        gate_pre, up_pre = s[:, :hid], s[:, hid:]
        sig = 1.0 / (1.0 + jnp.exp(-gate_pre))
        sw = gate_pre * sig
        hidden = (sw * up_pre).astype(BF)
        hiddens[at_chunk(h), :] = hidden
        slope = up_pre * sig * (1.0 + gate_pre * (1.0 - sig))
        for late in lates:
            ar(nb - 1, k, v, 1, late).wait_recv()
        proj = psy[h] + ary[nb - 1, h].astype(F32)
        route = jnp.sum(hidden.astype(F32) * proj, axis=1, keepdims=True)
        d1 = (proj * slope).astype(BF)
        d2 = (proj * sw).astype(BF)
        deltas[at_chunk(h), 0:hid] = d1
        deltas[at_chunk(h), hid:] = d2
        both = jnp.concatenate([d1, d2], axis=1)
        for m, at in enumerate(cols):
            part = lax.dot_general(
                both, wab[at, :], (((1,), (1,)), ((), ())), preferred_element_type=F32)
            rp[h, :, :, at] = part.reshape(2, half, part.shape[1]).astype(BF)
            if middle:
                to_middle(h, v, m).start()
            elif k:
                start_back(k, m, v)
        rsend[h] = jnp.broadcast_to(route, (chunk, LANES)).reshape(2, n_dp, CAP, LANES).astype(BF)
        for l in range(2):
            @pl.when(h * 2 + l != e)
            def _():
                rc(rsend.at[h, l, g], rret.at[e], rts, rtr, ep=h * 2 + l).start()

            @pl.when(h * 2 + l == e)
            def _():
                rret[e] = rsend[h, l, g]

    def send_back(k, v):
        h = v * per + at_order(k)
        for m, at in enumerate(cols):
            for ci in reversed(range(n_pair)):
                c = pair_at(ci)
                r1(h, c, m).wait_recv()
                both = rp[h, lo, pair_rows(c), at].astype(F32) + r1recv[h, pair_rows(c), at].astype(F32)
                r2send[h, pl.ds(2 * c, 2), :, at] = both.reshape(2, CAP, both.shape[1]).astype(BF)
                for b in range(2):
                    gp = 2 * c + b

                    def pass_on():
                        rc(r2send.at[h, gp, :, at], ret.at[hi * n_dp + g, :, at], r2s, r2r,
                           dp=gp, ep=h * 2 + lo).start()

                    def keep():
                        ret[hi * n_dp + g, :, at] = r2send[h, gp, :, at]

                    if ci or (k and experts == 1):
                        pass_on()
                    else:
                        mine = (h == hi) & (gp == g)
                        pl.when(jnp.logical_not(mine))(pass_on)
                        pl.when(mine)(keep)

    def G(s, *qs):
        over(functools.partial(gather_step, s, qs))

    def X(k, q, away):
        over(functools.partial(cross_on, k, q, away))

    def P(k, late=None):
        over(functools.partial(project, k, late))

    def A(k, late=None):
        for b in range(nb - 1):
            over(functools.partial(reduce_step, k, b, late))

    def F(k, *lates, middle=False):
        over(functools.partial(finish, k, lates or (None,), middle))

    def S(k, *parts):
        for m in parts:
            over(functools.partial(start_back, k, m))

    def R(k):
        over(functools.partial(send_back, k))

    tile = 256 if lw % 256 == 0 else 128
    tiles = lw // tile

    def wgrad(i, carry):
        ds = pl.ds(pl.multiple_of(i * tile, LANES), tile)
        dn = (((0,), (0,)), ((), ()))
        both = lax.dot_general(xs[:, ds], deltas[...], dn, preferred_element_type=F32).astype(BF)
        ga[ds, :] = both[:, :hid]
        gb[ds, :] = both[:, hid:]
        gc[ds, :] = lax.dot_general(ys[:, ds], hiddens[...], dn, preferred_element_type=F32).astype(BF)
        return carry

    def W(part):
        lax.fori_loop((0, (tiles + 1) // 2)[part], ((tiles + 1) // 2, tiles)[part], wgrad, 0)

    G(1, 0, 1)
    P(0)
    A(0)

    @pl.when(inner)
    def _():
        P(1, False)
        G(2, 0)
        A(1, False)
        X(2, 0, 0)
        P(1, True)
        G(2, 1)
        F(0)
        A(1, True)
        P(3, False)
        P(2)
        A(3, False)
        X(3, 1, 1)
        P(3, True)
        A(3, True)
        F(1, False, True, middle=True)
        A(2)
        F(3, False, True)
        F(2)
        R(3)
        over(merge)
        W(0)
        R(2)
        W(1)
        R(0)

    @pl.when(jnp.logical_not(inner))
    def _():
        G(2, 0, 1)
        P(1)
        A(1)
        F(0)
        G(3, 0)
        P(2, False)
        A(2, False)
        P(2, True)
        G(3, 1)
        S(0, 0)
        P(3, False)
        A(2, True)
        F(1)
        A(3, False)
        P(3, True)
        A(3, True)
        F(2, False, True)
        R(1)
        F(3, False, True)
        W(0)
        R(2)
        S(0, 1)
        R(3)
        R(0)
        W(1)

    def settle(ref, sem):
        pltpu.make_async_copy(ref, ref, sem).wait()

    def settle_back(sem):
        for group, fewer in ((inner, experts * n_dp), (jnp.logical_not(inner), 0)):
            @pl.when(group)
            def _():
                settle(ret.at[pl.ds(0, n_hi * n_dp - 1 - fewer)], sem)

    routes = rret.at[pl.ds(0, n_ep - 1)]
    settle_back(r2r)
    settle(routes, rtr)
    settle_back(r2s)
    settle(routes, rts)

    @pl.when(inner)
    def _():
        settle(r1recv.at[pl.ds(0, n_hi - experts)], r1s)
        settle(midrecv, mds)
        for w in range(experts):
            unused = (w * per + per - 1 - pos) * n_dp
            ret[pl.ds(unused, n_dp)] = jnp.zeros((n_dp, CAP, lw), BF)

    @pl.when(jnp.logical_not(inner))
    def _():
        settle(r1recv, r1s)

    settle(asx, asxs)
    settle(asy, asys)
    settle(xs.at[pl.ds(0, PAIR * (n_dp * experts - 1)), :], s1s)
    K = 2 * n_pair
    for at in range(per):
        ends = at in (0, per - 1)
        down = per - 1 - at
        crossing = lambda behind: n_pair if behind else K
        sent = (
            (sus, (at + 1) * K + crossing(at) if down else 0),
            (sds, (down + 1) * K + crossing(down) if at else 0),
            (sfs, (per - 1 if ends else per - 2) * K + n_pair),
        )

        @pl.when(pos == at)
        def _(sent=sent):
            for sem, count in sent:
                if count:
                    settle(xs.at[pl.ds(0, PAIR * count * experts), :], sem)


def finish_kernel(
    ret, rret, sel_ref, ga, gb, gc, ids_ref, rw_ref, ig_hbm, rg_ref, ga_out, gb_out, gc_out,
    obuf, sem_out, osem,
):
    per = SLICES // 2
    experts = rret.shape[0] // SLICES
    n_dp = ret.shape[0] // (experts * per)
    lw = ret.shape[2]
    rows = sel_ref.shape[1]
    stride = ROUTED // experts
    outs = [
        pltpu.make_async_copy(src, dst, sem_out.at[i])
        for i, (src, dst) in enumerate(((ga, ga_out), (gb, gb_out), (gc, gc_out)))
    ]
    for c in outs:
        c.start()
    sel = sel_ref[...]
    picks = sel.astype(BF)

    def total(ref, base, step, count):
        parts = []
        for w in range(experts):
            acc = ref[w * count * step + base].astype(F32)
            for i in range(1, count):
                acc = acc + ref[(w * count + i) * step + base].astype(F32)
            parts.append(acc)
        return jnp.concatenate(parts, axis=0) if experts > 1 else parts[0]

    ocopies = []
    for j in range(n_dp):
        obuf[:, j * lw:(j + 1) * lw] = lax.dot_general(
            picks, total(ret, j, n_dp, per).astype(BF), (((0,), (0,)), ((), ())),
            preferred_element_type=F32).astype(BF)
        ds = pl.ds(j * lw, lw)
        c = pltpu.make_async_copy(obuf.at[:, ds], ig_hbm.at[:, ds], osem.at[j])
        c.start()
        ocopies.append(c)
    terms = sel * total(rret, 0, 1, SLICES)
    ids = ids_ref[...]
    rg = jnp.zeros((TOPK, rows), F32)
    for w in range(experts):
        v = jnp.sum(terms[w * CAP:(w + 1) * CAP], axis=0, keepdims=True)
        rg = rg + jnp.where(ids == w * stride, v, 0.0)
    rg_ref[...] = rg / rw_ref[...].astype(F32)
    for c in outs + ocopies:
        c.wait()


def body(tokens, out_grad, expert_ids, route_weights, gate_matrix, up_matrix, down_matrix):
    n_dp, n_ep = lax.axis_size("dp"), lax.axis_size("ep")
    experts = n_ep // SLICES
    n_hi = n_ep // 2
    n_pair, per = n_dp // 2, SLICES // 2
    rows, width = tokens.shape
    lw, hid = gate_matrix.shape
    nb = n_dp.bit_length() - 1
    chunk = 2 * n_dp * CAP
    half = n_dp * CAP
    total = n_hi * chunk
    K = 2 * n_pair
    V = pltpu.VMEM
    D = lambda *s: pltpu.SemaphoreType.DMA(s)
    anyspec = pl.BlockSpec(memory_space=pl.ANY)
    vspec = pl.BlockSpec(memory_space=pltpu.VMEM)
    ids, rw = expert_ids.T, route_weights.T
    grad = jax.ShapeDtypeStruct((lw, hid), BF)
    kept = pl.pallas_call(
        functools.partial(kernel, n_dp, n_ep),
        out_shape=(
            V((n_hi * n_dp, CAP, lw), BF), V((n_ep, CAP, LANES), BF), V((experts * CAP, rows), F32),
            V((lw, hid), BF), V((lw, hid), BF), V((lw, hid), BF),
        ),
        in_specs=[anyspec] * 7,
        out_specs=(vspec,) * 6,
        scratch_shapes=[
            V((TOPK, rows), jnp.int32), V((TOPK, rows), BF),
            V((n_dp, rows, lw), BF), V((n_dp, rows, lw), BF), V((lw, 3 * hid), BF),
            V((n_dp, experts, CAP, 2 * lw), BF), V((experts, n_dp, CAP, 2 * lw), BF),
            V((total, lw), BF), V((total, lw), BF),
            V((n_hi, chunk, 2 * hid), F32), V((n_hi, chunk, hid), F32),
            V((nb, n_hi, chunk, 2 * hid), BF), V((nb, n_hi, chunk, 2 * hid), BF),
            V((nb, n_hi, chunk, hid), BF), V((nb, n_hi, chunk, hid), BF),
            V((total, 2 * hid), BF), V((total, hid), BF),
            V((n_hi, 2, half, lw), BF), V((n_hi, half, lw), BF), V((n_hi, n_dp, CAP, lw), BF),
            V((experts, 2, half, lw), BF),
            V((n_hi, 2, n_dp, CAP, LANES), BF),
            D(2, n_dp), D(2), D(13), D(2, experts, n_dp), D(n_hi, K), D(n_hi, K), D(nb, n_hi, 2), D(nb, per - 1, experts, 2), D(n_hi, n_pair, 2), D(experts, 2),
        ],
        compiler_params=pltpu.CompilerParams(
            collective_id=0, has_side_effects=True, vmem_limit_bytes=VMEM_BYTES),
    )(tokens, out_grad, ids, rw, gate_matrix, up_matrix, down_matrix)
    kept = [pltpu.with_memory_space_constraint(a, pltpu.VMEM) for a in kept]
    ig, rg, ga, gb, gc = pl.pallas_call(
        finish_kernel,
        out_shape=(
            jax.ShapeDtypeStruct((rows, width), BF),
            jax.ShapeDtypeStruct((TOPK, rows), F32),
            grad, grad, grad,
        ),
        in_specs=[vspec] * 8,
        out_specs=(anyspec, vspec, anyspec, anyspec, anyspec),
        scratch_shapes=[V((rows, width), BF), D(3), D(n_dp)],
        compiler_params=pltpu.CompilerParams(vmem_limit_bytes=16 * 1024 * 1024),
    )(*kept, ids, rw)
    return ig, rg.T, ga, gb, gc


def solution(mesh):
    return jax.shard_map(
        body,
        mesh=mesh,
        in_specs=(
            P(("dp", "ep"), None),
            P(("dp", "ep"), None),
            P(("dp", "ep"), None),
            P(("dp", "ep"), None),
            P("dp", "ep"),
            P("dp", "ep"),
            P("dp", "ep"),
        ),
        out_specs=(
            P(("dp", "ep"), None),
            P(("dp", "ep"), None),
            P("dp", "ep"),
            P("dp", "ep"),
            P("dp", "ep"),
        ),
        check_vma=False,
    )
```
